32 devices in a mesh: seq: 32 (over z, y, x, core).
Axes of the slice: x: 2, y: 2, z: 4, core: 2. Of those that a mesh axis runs over, the one named last changes fastest.
Arguments:
- queries: bfloat16 [32768, 4096], P('seq'), may hold values from -6 to 6
- span_keys: bfloat16 [32768, 1024], P('seq'), may hold values from -6 to 6
- span_values: bfloat16 [32768, 1024], P('seq'), may hold values from -6 to 6
- past_keys: bfloat16 [2, 32, 512, 1024], P(None, 'seq'), may hold values from -6 to 6
- past_values: bfloat16 [2, 32, 512, 1024], P(None, 'seq'), may hold values from -6 to 6
- selected: int32 [64, 8, 4], P('seq'), may hold values from 0 to 63, as said below
Outputs:
- attended: bfloat16 [32768, 4096], P('seq')
The draws below stay inside these ranges and needn't reach their ends.
Inputs may be any that keep to these rules, and one draw needn't show every extreme that they name: `selected`: query blocks k * 2 to (k + 1) * 2 - 1 form group k. Among the 64 numbers of one group, at most 2 are equal modulo 32, and some residue is named exactly 2 times.
All inputs are finite; a program needn't handle non-finite values.
Results may differ from the reference program's by a relative error of at most 0.005.
Values may be sent and summed in bfloat16 or wider, within the bound.
A program may use at most 256 MiB of HBM per device.

```python
import jax
import jax.numpy as jnp
from jax import lax

QH = 32
KVH = 8
HD = 128
BLOCK = 512
TOPK = 4
QB_DEV = 2
PB_DEV = 2
QTOK = 32768
N_SEQ = 32


def draw_queries(key, part):
    rows = BLOCK * QB_DEV * N_SEQ
    base = jnp.clip(jax.random.normal(jax.random.fold_in(key, 1), (rows, QH * HD), jnp.float32), -6.0, 6.0)
    return base.astype(jnp.bfloat16)


def draw_past_keys(key, part):
    base = jnp.clip(jax.random.normal(jax.random.fold_in(key, 5), (PB_DEV, N_SEQ, BLOCK, KVH * HD), jnp.float32), -6.0, 6.0)
    return base.astype(jnp.bfloat16)


def draw_selected(key, part):
    needed = QB_DEV * KVH * TOPK
    copies = (needed + N_SEQ - 1) // N_SEQ
    pool = jnp.tile(jnp.arange(N_SEQ, dtype=jnp.int32), copies)
    order_keys = jax.random.split(jax.random.fold_in(key, 11), N_SEQ)
    orders = jax.vmap(lambda item: jax.random.permutation(item, pool))(order_keys)
    owners = orders[:, :needed].reshape(N_SEQ * QB_DEV, KVH, TOPK).astype(jnp.int32)
    popular = jax.random.randint(jax.random.fold_in(key, 12), (N_SEQ,), 0, PB_DEV)
    favour = jax.random.randint(jax.random.fold_in(key, 13), (N_SEQ * QB_DEV, KVH, TOPK), 0, 10) < 6
    others = jax.random.randint(jax.random.fold_in(key, 14), (N_SEQ * QB_DEV, KVH, TOPK), 0, PB_DEV)
    local = jnp.where(favour, popular[owners], others)
    return (local * N_SEQ + owners).astype(jnp.int32)


def block_levels(key, shape, pieces, low, largest):
    gain = 1.0
    for dim, blocks in pieces:
        steps = jax.random.uniform(jax.random.fold_in(jax.random.fold_in(key, 6), dim), (blocks,), jnp.float32, low / len(pieces), largest / len(pieces))
        gain = gain * jnp.repeat(jnp.exp(steps), shape[dim] // blocks).reshape((-1,) + (1,) * (len(shape) - 1 - dim))
    return gain


def normal_values(rng, shape, scale, reach, cuts=(), kind=jnp.bfloat16):
    array = jax.random.normal(rng, shape, jnp.float32) * scale
    if len(cuts) > 0:
        array = block_levels(rng, shape, cuts, -0.22, 0.18) * array
    return jnp.clip(array, min=-reach, max=reach).astype(kind)


def setup_inputs(seed: int = 0) -> dict:
    arg_keys = jax.random.split(jax.random.key(seed), 7)
    queries = draw_queries(jax.random.fold_in(arg_keys[6], 71), 0)
    span_keys = normal_values(arg_keys[1], (QTOK, KVH * HD), 1.0, 6.0, ((0, 32),))
    span_values = normal_values(arg_keys[2], (QTOK, KVH * HD), 1.0, 6.0, ((0, 32),))
    past_keys = draw_past_keys(jax.random.fold_in(arg_keys[6], 71), 0)
    past_values = normal_values(arg_keys[4], (PB_DEV, N_SEQ, BLOCK, KVH * HD), 1.0, 6.0, ((1, 32),))
    selected = draw_selected(jax.random.fold_in(arg_keys[6], 71), 0)
    return dict(queries=queries, span_keys=span_keys, span_values=span_values, past_keys=past_keys, past_values=past_values, selected=selected)


def reference(queries, span_keys, span_values, past_keys, past_values, selected):
    group = QH // KVH
    scale = HD ** -0.5
    blocks_all = QB_DEV * N_SEQ
    query_blocks = queries.reshape(blocks_all, BLOCK, KVH, group, HD)
    near_keys_all = span_keys.reshape(blocks_all, BLOCK, KVH, HD)
    near_values_all = span_values.reshape(blocks_all, BLOCK, KVH, HD)
    far_keys_all = past_keys.reshape(PB_DEV * N_SEQ, BLOCK, KVH, HD)
    far_values_all = past_values.reshape(PB_DEV * N_SEQ, BLOCK, KVH, HD)
    head_ids = jnp.arange(KVH, dtype=jnp.int32)[:, None]
    causal = jnp.arange(BLOCK)[None, :] <= jnp.arange(BLOCK)[:, None]

    def one_block(items):
        query_block, near_keys, near_values, chosen = items
        far_keys = far_keys_all[chosen, :, head_ids, :].reshape(KVH, TOPK * BLOCK, HD).astype(jnp.float32)
        far_values = far_values_all[chosen, :, head_ids, :].reshape(KVH, TOPK * BLOCK, HD).astype(jnp.float32)
        query_wide = query_block.astype(jnp.float32)
        far = jnp.einsum("ihgd,hkd->hgik", query_wide, far_keys) * scale
        near = jnp.einsum("ihgd,jhd->hgij", query_wide, near_keys.astype(jnp.float32)) * scale
        near = jnp.where(causal, near, -jnp.inf)
        top = jnp.maximum(jnp.max(far, axis=-1), jnp.max(near, axis=-1))[..., None]
        far_weight = jnp.exp(far - top)
        near_weight = jnp.exp(near - top)
        total = jnp.sum(far_weight, axis=-1, keepdims=True) + jnp.sum(near_weight, axis=-1, keepdims=True)
        far_probs = (far_weight / total).astype(jnp.bfloat16).astype(jnp.float32)
        near_probs = (near_weight / total).astype(jnp.bfloat16).astype(jnp.float32)
        result = jnp.einsum("hgik,hkd->ihgd", far_probs, far_values)
        result = result + jnp.einsum("hgij,jhd->ihgd", near_probs, near_values.astype(jnp.float32))
        return result.astype(jnp.bfloat16).reshape(BLOCK, QH * HD)

    attended = lax.map(one_block, (query_blocks, near_keys_all, near_values_all, selected))
    return attended.reshape(blocks_all * BLOCK, QH * HD)
```

```python
import functools
import math

import jax
import jax.numpy as jnp
from jax import lax
from jax.experimental import pallas as pl
from jax.experimental.pallas import tpu as pltpu
from jax.sharding import PartitionSpec as P


GROUPS = 8


def owner_ranks(owners):
    length = owners.shape[-1]
    later = lax.broadcasted_iota(jnp.int32, (length, length), 0)
    sooner = lax.broadcasted_iota(jnp.int32, (length, length), 1)
    same = owners[..., :, None] == owners[..., None, :]
    return jnp.sum(jnp.where(same & (sooner < later), 1, 0), axis=-1).astype(jnp.int32)


def gather_kernel(count, slots, heads, width, request_ref, keys_ref, values_ref, *rest):
    outs, sems = rest[:count], rest[count]
    copies = []
    for turn in range(count):
        for slot in range(slots):
            request = request_ref[turn * slots + slot]
            block, head = request // heads, lax.rem(request, heads)
            lanes = pl.ds(pl.multiple_of(head * width, width), width)
            for kind, ref in ((0, keys_ref), (1, values_ref)):
                copy = pltpu.make_async_copy(
                    ref.at[block, 0, :, lanes],
                    outs[turn].at[slot, kind],
                    sems.at[turn * slots * 2 + slot * 2 + kind],
                )
                copy.start()
                copies.append(copy)
    for copy in copies:
        copy.wait()


def gather_requests(request, past_keys, past_values, count, slots, heads):
    block, width = past_keys.shape[2], past_keys.shape[3] // heads
    piece = jax.ShapeDtypeStruct((slots, 2, block, width), past_keys.dtype)
    return pl.pallas_call(
        functools.partial(gather_kernel, count, slots, heads, width),
        out_shape=[piece] * count,
        in_specs=[
            pl.BlockSpec(memory_space=pltpu.SMEM),
            pl.BlockSpec(memory_space=pltpu.VMEM),
            pl.BlockSpec(memory_space=pltpu.VMEM),
        ],
        out_specs=[pl.BlockSpec(memory_space=pl.ANY)] * count,
        scratch_shapes=[pltpu.SemaphoreType.DMA((count * slots * 2,))],
    )(request, past_keys, past_values)


def partial_attention(query_ref, keys, values, out_ref, stat_ref, group, mask):
    block, width = keys.shape
    factor = width**-0.5 * math.log2(math.e)
    values_t = values.T
    for member in range(group):
        query = query_ref[:, member * width : (member + 1) * width]
        span = slice(member * block, (member + 1) * block)
        scores = lax.dot_general(
            keys, query, (((1,), (1,)), ((), ())), preferred_element_type=jnp.float32
        )
        if mask is not None:
            scores = jnp.where(mask, scores, -jnp.inf)
        top = jnp.max(scores, axis=0, keepdims=True) * factor
        weights = jnp.exp2(scores * factor - top)
        stat_ref[0, 0:1, span] = top
        stat_ref[0, 1:2, span] = jnp.sum(weights, axis=0, keepdims=True)
        out_ref[0, :, span] = jnp.dot(
            values_t, weights.astype(jnp.bfloat16), preferred_element_type=jnp.float32
        ).astype(jnp.bfloat16)


def near_kernel(group, query_ref, keys_ref, values_ref, out_ref, stat_ref):
    block = keys_ref.shape[0]
    mask = lax.broadcasted_iota(jnp.int32, (block, block), 0) <= lax.broadcasted_iota(
        jnp.int32, (block, block), 1
    )
    partial_attention(
        query_ref, keys_ref[...], values_ref[...], out_ref, stat_ref, group, mask
    )


def far_kernel(group, rows_ref, query_ref, pair_ref, _out, _stat, out_ref, stat_ref):
    partial_attention(
        query_ref, pair_ref[0, 0], pair_ref[0, 1], out_ref, stat_ref, group, None
    )


def merge_kernel(group, picks, places_ref, *refs):
    outs, stats, result_ref = refs[: picks + 1], refs[picks + 1 : 2 * picks + 2], refs[-1]
    width = outs[0].shape[1]
    block = result_ref.shape[0]
    for member in range(group):
        span = slice(member * block, (member + 1) * block)
        tops = [stat[0, 0:1, span] for stat in stats]
        top = functools.reduce(jnp.maximum, tops)
        scales = [jnp.exp2(item - top) for item in tops]
        total = sum(scale * stat[0, 1:2, span] for scale, stat in zip(scales, stats))
        inverse = 1.0 / total
        mixed = sum(
            out[0, :, span].astype(jnp.float32) * (scale * inverse)
            for out, scale in zip(outs, scales)
        )
        result_ref[:, member * width : (member + 1) * width] = mixed.T.astype(jnp.bfloat16)


def plain_shards(queries, span_keys, span_values, past_keys, past_values, selected):
    count = lax.axis_size("seq")
    me = lax.axis_index("seq")
    local_blocks, heads, picks = selected.shape
    needed = local_blocks * heads * picks
    rows = local_blocks * heads
    slots = (needed + count - 1) // count
    block = queries.shape[0] // local_blocks
    width = past_keys.shape[-1] // heads
    group = queries.shape[1] // (heads * width)
    span = group * block

    chosen = selected.reshape(-1)
    owners = chosen % count
    ranks = owner_ranks(owners)
    head_flat = lax.broadcasted_iota(jnp.int32, selected.shape, 1).reshape(-1)
    wanted = chosen // count * heads + head_flat
    slot_ids = owners * slots + ranks
    match = slot_ids[None, :] == jnp.arange(count * slots, dtype=jnp.int32)[:, None]
    outgoing = jnp.sum(jnp.where(match, wanted[None, :], 0), axis=1).reshape(count, slots)
    incoming = lax.all_to_all(outgoing, "seq", split_axis=0, concat_axis=0, tiled=True)

    turns = [0]
    for step in range(1, count // 2 + 1):
        turns.append(step)
        if step != count - step:
            turns.append(count - step)
    turns_array = jnp.array(turns, dtype=jnp.int32)
    request = jnp.take(incoming, (me + turns_array) % count, axis=0).reshape(-1)
    sources = (me - turns_array) % count
    place_ids = (sources[:, None] * slots + jnp.arange(slots, dtype=jnp.int32)).reshape(-1)
    found = place_ids[:, None] == slot_ids[None, :]
    pick_rows = jnp.arange(needed, dtype=jnp.int32) // picks
    pair_rows = jnp.sum(jnp.where(found, pick_rows[None, :], 0), axis=1).astype(jnp.int32)
    place_of = jnp.sum(
        jnp.where(found, jnp.arange(count * slots, dtype=jnp.int32)[:, None], 0), axis=0
    ).astype(jnp.int32)

    pieces = gather_requests(request, past_keys, past_values, count, slots, heads)
    arrived = [pieces[0]]
    for turn, piece in zip(turns[1:], pieces[1:]):
        arrived.append(
            lax.ppermute(piece, "seq", [(d, (d + turn) % count) for d in range(count)])
        )

    places = count * slots + rows
    partial_shapes = [
        jax.ShapeDtypeStruct((places, width, span), jnp.bfloat16),
        jax.ShapeDtypeStruct((places, 2, span), jnp.float32),
    ]
    pair_cost = 4 * span * block * width
    outs, stats = pl.pallas_call(
        functools.partial(near_kernel, group),
        grid=(rows,),
        in_specs=[
            pl.BlockSpec((block, group * width), lambda i: (i // heads, i % heads)),
            pl.BlockSpec((block, width), lambda i: (i // heads, i % heads)),
            pl.BlockSpec((block, width), lambda i: (i // heads, i % heads)),
        ],
        out_specs=[
            pl.BlockSpec((1, width, span), lambda i: (i + count * slots, 0, 0)),
            pl.BlockSpec((1, 2, span), lambda i: (i + count * slots, 0, 0)),
        ],
        out_shape=partial_shapes,
        cost_estimate=pl.CostEstimate(
            flops=rows * pair_cost, bytes_accessed=rows * 1500000, transcendentals=0
        ),
    )(queries, span_keys, span_values)

    size = max(count // GROUPS, 1)
    for first in range(0, count, size):
        pairs = jnp.concatenate(arrived[first : first + size], axis=0)
        length = pairs.shape[0]
        base = first * slots
        outs, stats = pl.pallas_call(
            functools.partial(far_kernel, group),
            grid_spec=pltpu.PrefetchScalarGridSpec(
                num_scalar_prefetch=1,
                grid=(length,),
                in_specs=[
                    pl.BlockSpec(
                        (block, group * width),
                        lambda i, r: (r[i] // heads, lax.rem(r[i], heads)),
                    ),
                    pl.BlockSpec((1, 2, block, width), lambda i, r: (i, 0, 0, 0)),
                    pl.BlockSpec(memory_space=pl.ANY),
                    pl.BlockSpec(memory_space=pl.ANY),
                ],
                out_specs=[
                    pl.BlockSpec((1, width, span), lambda i, r, base=base: (i + base, 0, 0)),
                    pl.BlockSpec((1, 2, span), lambda i, r, base=base: (i + base, 0, 0)),
                ],
            ),
            out_shape=partial_shapes,
            input_output_aliases={3: 0, 4: 1},
            cost_estimate=pl.CostEstimate(
                flops=length * pair_cost, bytes_accessed=length * 1500000, transcendentals=0
            ),
        )(lax.dynamic_slice_in_dim(pair_rows, base, length), queries, pairs, outs, stats)

    def far_place(pick):
        return lambda i, p: (p[i * picks + pick], 0, 0)

    maps = [far_place(pick) for pick in range(picks)]
    maps.append(lambda i, p: (i + count * slots, 0, 0))
    return pl.pallas_call(
        functools.partial(merge_kernel, group, picks),
        grid_spec=pltpu.PrefetchScalarGridSpec(
            num_scalar_prefetch=1,
            grid=(rows,),
            in_specs=[pl.BlockSpec((1, width, span), item) for item in maps]
            + [pl.BlockSpec((1, 2, span), item) for item in maps],
            out_specs=pl.BlockSpec(
                (block, group * width), lambda i, p: (i // heads, i % heads)
            ),
        ),
        out_shape=jax.ShapeDtypeStruct(queries.shape, queries.dtype),
    )(place_of, *([outs] * (picks + 1)), *([stats] * (picks + 1)))


MESH = pl.DeviceIdType.MESH
CHUNKS = 4
VMEM_BYTES = 65_000_000


def crossed(a, b, bits):
    total = 0
    for bit in range(bits):
        total = total + (a // 2**bit + b // 2**bit) % 2 * 2**bit
    return total


def attend(take_query, keys, values, store_out, store_stat, group, mask):
    block, width = keys.shape
    factor = width**-0.5 * math.log2(math.e)
    values_t = values.T
    for member in range(group):
        scores = lax.dot_general(
            keys,
            take_query(member),
            (((1,), (1,)), ((), ())),
            preferred_element_type=jnp.float32,
        )
        if mask is not None:
            scores = jnp.where(mask, scores, -jnp.inf)
        top = jnp.max(scores, axis=0, keepdims=True) * factor
        weights = jnp.exp2(scores * factor - top)
        store_stat(member, top, jnp.sum(weights, axis=0, keepdims=True))
        store_out(
            member,
            jnp.dot(
                values_t, weights.astype(jnp.bfloat16), preferred_element_type=jnp.float32
            ).astype(jnp.bfloat16),
        )


def exchange_kernel(
    heads,
    group,
    slots,
    ask_ref,
    rows_ref,
    queries_hbm,
    span_keys_hbm,
    span_values_hbm,
    past_keys_hbm,
    past_values_hbm,
    outs_hbm,
    stats_ref,
    query,
    near_keys,
    near_values,
    own,
    stage_own,
    stage_far,
    got_own,
    got_far,
    out_buf,
    told,
    told_scalar,
    *rest,
):
    mirror, sems = rest[:CHUNKS], rest[CHUNKS:]
    (load_sem, query_sem, out_sem, tell_send, tell_recv, tell_local, copy_send, copy_recv) = sems[:8]
    (own_send, own_recv, far_send, far_recv) = sems[8:]
    count = lax.axis_size("seq")
    me = lax.axis_index("seq")
    half = ask_ref.shape[0]
    bits = half.bit_length() - 1
    local = me % half
    base = me - local
    partner = (me + half) % count
    local_blocks = past_keys_hbm.shape[0]
    block, width = got_own.shape[-2:]
    part = block // CHUNKS
    rows = outs_hbm.shape[0] - count * slots

    def peer(turn):
        return base + crossed(local, turn, bits)

    def load_own(kind, head):
        source = (past_keys_hbm, past_values_hbm)[kind]
        lanes = pl.ds(pl.multiple_of(head * width, width), width)
        return pltpu.make_async_copy(
            source.at[:, 0, :, lanes], own.at[kind, :, head], load_sem.at[kind, head]
        )

    def load_near(kind, head):
        source, target = ((span_keys_hbm, near_keys), (span_values_hbm, near_values))[kind]
        lanes = pl.ds(pl.multiple_of(head * width, width), width)
        return pltpu.make_async_copy(
            source.at[:, :, lanes], target.at[head], load_sem.at[2 + kind, head]
        )

    def load_query(item):
        lanes = pl.ds(pl.multiple_of(item * width, width), width)
        return pltpu.make_async_copy(
            queries_hbm.at[:, :, lanes], query.at[item], query_sem.at[item]
        )

    def each_head(body):
        def step(head, carry):
            for kind in range(2):
                body(kind, head)
            return carry

        lax.fori_loop(0, heads, step, 0)

    def each_query(body):
        def step(item, carry):
            body(item)
            return carry

        lax.fori_loop(0, heads * group, step, 0)

    each_head(lambda kind, head: load_own(kind, head).start())
    each_head(lambda kind, head: load_near(kind, head).start())
    each_query(lambda item: load_query(item).start())

    barrier = pltpu.get_barrier_semaphore()

    def greet(turn, carry):
        pl.semaphore_signal(barrier, inc=1, device_id=(peer(turn),), device_id_type=MESH)
        return carry

    lax.fori_loop(1, half, greet, 0)
    pl.semaphore_signal(barrier, inc=1, device_id=(partner,), device_id_type=MESH)
    pl.semaphore_wait(barrier, half)

    def tell(turn):
        return pltpu.make_async_remote_copy(
            src_ref=ask_ref.at[turn],
            dst_ref=told.at[turn],
            send_sem=tell_send.at[turn],
            recv_sem=tell_recv.at[turn],
            device_id=(peer(turn),),
            device_id_type=MESH,
        )

    def mirror_copy(chunk, kind):
        return pltpu.make_async_remote_copy(
            src_ref=own.at[kind, :, :, pl.ds(chunk * part, part), :],
            dst_ref=mirror[chunk].at[kind],
            send_sem=copy_send.at[chunk * 2 + kind],
            recv_sem=copy_recv.at[chunk * 2 + kind],
            device_id=(partner,),
            device_id_type=MESH,
        )

    def send_own(turn):
        return pltpu.make_async_remote_copy(
            src_ref=stage_own.at[turn],
            dst_ref=got_own.at[turn],
            send_sem=own_send.at[turn],
            recv_sem=own_recv.at[turn],
            device_id=(peer(turn),),
            device_id_type=MESH,
        )

    def send_far(chunk, turn):
        span = pl.ds(chunk * part, part)
        return pltpu.make_async_remote_copy(
            src_ref=stage_far.at[turn, :, :, span, :],
            dst_ref=got_far.at[turn, :, :, span, :],
            send_sem=far_send.at[chunk, turn],
            recv_sem=far_recv.at[chunk, turn],
            device_id=(peer(turn),),
            device_id_type=MESH,
        )

    def each_turn(first, body):
        def step(turn, carry):
            body(turn)
            return carry

        lax.fori_loop(first, half, step, 0)

    def each_turn_down(body):
        def step(item, carry):
            body(half - 1 - item)
            return carry

        lax.fori_loop(0, half - 1, step, 0)

    each_turn(1, lambda turn: tell(turn).start())
    each_head(lambda kind, head: load_own(kind, head).wait())
    for chunk in range(CHUNKS):
        for kind in range(2):
            mirror_copy(chunk, kind).start()

    each_turn(1, lambda turn: tell(turn).wait_recv())
    own_row = pltpu.make_async_copy(ask_ref.at[0], told_scalar.at[0], tell_local.at[0])
    other_rows = pltpu.make_async_copy(
        told.at[pl.ds(1, half - 1)], told_scalar.at[pl.ds(1, half - 1)], tell_local.at[1]
    )
    own_row.start()
    other_rows.start()
    own_row.wait()
    other_rows.wait()
    def wanted(turn, slot):
        return told_scalar[turn, 0, slot], told_scalar[turn, 0, 2 * slots + slot]

    def gather_own(store, turn):
        for slot in range(slots):
            which, head = wanted(turn, slot)
            for kind in range(2):
                store[turn, slot, kind] = own[kind, which, head]

    def gather_far(chunk, store, turn):
        for slot in range(slots):
            which, head = wanted(turn, slots + slot)
            for kind in range(2):
                store[turn, slot, kind, pl.ds(chunk * part, part), :] = mirror[chunk][
                    kind, which, head
                ]

    gather_own(got_own, 0)
    each_turn(1, functools.partial(gather_own, stage_own))
    each_turn_down(lambda turn: send_own(turn).start())

    def put_out(place, buffer):
        return pltpu.make_async_copy(out_buf.at[buffer], outs_hbm.at[place], out_sem.at[buffer])

    def pair(place, buffer, first, head, query_block, keys, values, mask):
        if first is not False:
            pl.when(jnp.logical_not(first))(put_out(place, buffer).wait)
        else:
            put_out(place, buffer).wait()

        def take_query(member):
            return query[head * group + member, query_block]

        def store_out(member, value):
            out_buf[buffer, :, pl.ds(member * block, block)] = value

        def store_stat(member, top, total):
            stats_ref[place, 0:1, pl.ds(member * block, block)] = top
            stats_ref[place, 1:2, pl.ds(member * block, block)] = total

        attend(take_query, keys, values, store_out, store_stat, group, mask)
        put_out(place, buffer).start()

    each_head(lambda kind, head: load_near(kind, head).wait())
    each_query(lambda item: load_query(item).wait())
    mask = lax.broadcasted_iota(jnp.int32, (block, block), 0) <= lax.broadcasted_iota(
        jnp.int32, (block, block), 1
    )

    def near_step(item, carry):
        for buffer in range(2):
            row = item * 2 + buffer
            query_block, head = row // heads, row % heads
            pair(
                count * slots + row,
                buffer,
                item == 0,
                head,
                query_block,
                near_keys[head, query_block],
                near_values[head, query_block],
                mask,
            )
        return carry

    lax.fori_loop(0, rows // 2, near_step, 0)

    def far_pair(turn, extra, slot, store):
        place = turn * (2 * slots) + extra + slot
        pair(
            place,
            slot % 2,
            False,
            rows_ref[count * slots + place],
            rows_ref[place],
            store[turn, slot, 0],
            store[turn, slot, 1],
            None,
        )

    def forward(chunk):
        for kind in range(2):
            mirror_copy(chunk, kind).wait_recv()
        gather_far(chunk, got_far, 0)
        each_turn(1, functools.partial(gather_far, chunk, stage_far))
        each_turn_down(lambda turn: send_far(chunk, turn).start())

    def own_step(item, carry):
        for chunk in range(CHUNKS):
            pl.when(item == chunk * (half // CHUNKS))(functools.partial(forward, chunk))

        middle = half // 2
        turn = jnp.where(
            item < middle - 1,
            half - item,
            jnp.where(item < half - 2, half - 2 - item, half + middle - 1 - item),
        )
        turn = jnp.where(item == 0, 0, turn)

        @pl.when(turn > 0)
        def _():
            send_own(turn).wait_recv()

        for slot in range(slots):
            far_pair(turn, 0, slot, got_own)
        return carry

    lax.fori_loop(0, half, own_step, 0)

    def far_step(item, carry):
        turn = jnp.where(item == 0, 0, half - item)

        @pl.when(turn > 0)
        def _():
            for chunk in range(CHUNKS):
                send_far(chunk, turn).wait_recv()

        for slot in range(slots):
            far_pair(turn, slots, slot, got_far)
        return carry

    lax.fori_loop(0, half, far_step, 0)

    for buffer in range(2):
        put_out(buffer, buffer).wait()
    each_turn(1, lambda turn: tell(turn).wait_send())
    each_turn(1, lambda turn: send_own(turn).wait_send())
    for chunk in range(CHUNKS):
        for kind in range(2):
            mirror_copy(chunk, kind).wait_send()
        each_turn(1, lambda turn: send_far(chunk, turn).wait_send())


def mirrored_shards(queries, span_keys, span_values, past_keys, past_values, selected):
    count = lax.axis_size("seq")
    me = lax.axis_index("seq")
    local_blocks, heads, picks = selected.shape
    needed = local_blocks * heads * picks
    rows = local_blocks * heads
    slots = needed // count
    half = count // 2
    block = queries.shape[0] // local_blocks
    width = past_keys.shape[-1] // heads
    group = queries.shape[1] // (heads * width)
    span = group * block
    kind = past_keys.dtype

    chosen = selected.reshape(-1)
    owners = chosen % count
    away = (owners // half != me // half).astype(jnp.int32)
    turns = (owners % half) ^ (me % half)
    places = turns * (2 * slots) + away * slots + owner_ranks(owners)
    found = jnp.arange(needed, dtype=jnp.int32)[:, None] == places[None, :]
    head_flat = lax.broadcasted_iota(jnp.int32, selected.shape, 1).reshape(-1)
    query_blocks = lax.broadcasted_iota(jnp.int32, selected.shape, 0).reshape(-1)

    def placed(values):
        return jnp.sum(jnp.where(found, values[None, :], 0), axis=1).astype(jnp.int32)

    place_heads = placed(head_flat)
    pair_rows = jnp.concatenate([placed(query_blocks), place_heads])
    ask = jnp.concatenate(
        [
            placed(chosen // count).reshape(half, 1, 2 * slots),
            place_heads.reshape(half, 1, 2 * slots),
            jnp.zeros((half, 1, 128 - 4 * slots), jnp.int32),
        ],
        axis=2,
    )

    total = count * slots + rows
    store = pltpu.VMEM((half, slots, 2, block, width), kind)
    dma = pltpu.SemaphoreType.DMA
    outs, stats = pl.pallas_call(
        functools.partial(exchange_kernel, heads, group, slots),
        in_specs=[
            pl.BlockSpec(memory_space=pltpu.VMEM),
            pl.BlockSpec(memory_space=pltpu.SMEM),
        ]
        + [pl.BlockSpec(memory_space=pl.ANY)] * 5,
        out_specs=[
            pl.BlockSpec(memory_space=pl.ANY),
            pl.BlockSpec(memory_space=pltpu.VMEM),
        ],
        out_shape=[
            jax.ShapeDtypeStruct((total, width, span), jnp.bfloat16),
            jax.ShapeDtypeStruct((total, 2, span), jnp.float32),
        ],
        scratch_shapes=[
            pltpu.VMEM((heads * group, local_blocks, block, width), queries.dtype),
            pltpu.VMEM((heads, local_blocks, block, width), span_keys.dtype),
            pltpu.VMEM((heads, local_blocks, block, width), span_values.dtype),
            pltpu.VMEM((2, past_keys.shape[0], heads, block, width), kind),
            store,
            store,
            store,
            store,
            pltpu.VMEM((2, width, span), jnp.bfloat16),
            pltpu.VMEM((half, 1, 128), jnp.int32),
            pltpu.SMEM((half, 1, 128), jnp.int32),
        ]
        + [pltpu.VMEM((2, past_keys.shape[0], heads, block // CHUNKS, width), kind)] * CHUNKS
        + [
            dma((4, heads)),
            dma((heads * group,)),
            dma((2,)),
            dma((half,)),
            dma((half,)),
            dma((2,)),
            dma((2 * CHUNKS,)),
            dma((2 * CHUNKS,)),
            dma((half,)),
            dma((half,)),
            dma((CHUNKS, half)),
            dma((CHUNKS, half)),
        ],
        compiler_params=pltpu.CompilerParams(
            collective_id=0, has_side_effects=True, vmem_limit_bytes=VMEM_BYTES
        ),
    )(
        ask,
        pair_rows,
        queries.reshape(local_blocks, block, -1),
        span_keys.reshape(local_blocks, block, -1),
        span_values.reshape(local_blocks, block, -1),
        past_keys,
        past_values,
    )

    def far_place(pick):
        return lambda i, p: (p[i * picks + pick], 0, 0)

    maps = [far_place(pick) for pick in range(picks)]
    maps.append(lambda i, p: (i + count * slots, 0, 0))
    return pl.pallas_call(
        functools.partial(merge_kernel, group, picks),
        grid_spec=pltpu.PrefetchScalarGridSpec(
            num_scalar_prefetch=1,
            grid=(rows,),
            in_specs=[pl.BlockSpec((1, width, span), item) for item in maps]
            + [pl.BlockSpec((1, 2, span), item) for item in maps],
            out_specs=pl.BlockSpec(
                (block, group * width), lambda i, p: (i // heads, i % heads)
            ),
        ),
        out_shape=jax.ShapeDtypeStruct(queries.shape, queries.dtype),
    )(places, *([outs] * (picks + 1)), *([stats] * (picks + 1)))


def shards(queries, span_keys, span_values, past_keys, past_values, selected):
    count = lax.axis_size("seq")
    needed = selected.size
    half = count // 2
    held = 2 * (queries.size + 2 * span_keys.size + 4 * past_keys.size)
    held += 16 * needed * past_keys.shape[2] * (past_keys.shape[3] // selected.shape[1]) // 2
    fits = held < VMEM_BYTES - 2**23
    whole = needed == count * max(needed // count, 1) and needed // max(count, 1) == 2
    if fits and whole and half >= 2 * CHUNKS and half & (half - 1) == 0:
        call = mirrored_shards
    else:
        call = plain_shards
    return call(queries, span_keys, span_values, past_keys, past_values, selected)


def solution(mesh):
    return jax.shard_map(
        shards,
        mesh=mesh,
        in_specs=(
            P("seq", None),
            P("seq", None),
            P("seq", None),
            P(None, "seq", None, None),
            P(None, "seq", None, None),
            P("seq", None, None),
        ),
        out_specs=P("seq", None),
        check_vma=False,
    )
```

```python
import functools
import math

import jax
import jax.numpy as jnp
from jax import lax
from jax.experimental import pallas as pl
from jax.experimental.pallas import tpu as pltpu
from jax.sharding import PartitionSpec as P


GROUPS = 8


def owner_ranks(owners):
    length = owners.shape[-1]
    later = lax.broadcasted_iota(jnp.int32, (length, length), 0)
    sooner = lax.broadcasted_iota(jnp.int32, (length, length), 1)
    same = owners[..., :, None] == owners[..., None, :]
    return jnp.sum(jnp.where(same & (sooner < later), 1, 0), axis=-1).astype(jnp.int32)


def gather_kernel(count, slots, heads, width, request_ref, keys_ref, values_ref, *rest):
    outs, sems = rest[:count], rest[count]
    copies = []
    for turn in range(count):
        for slot in range(slots):
            request = request_ref[turn * slots + slot]
            block, head = request // heads, lax.rem(request, heads)
            lanes = pl.ds(pl.multiple_of(head * width, width), width)
            for kind, ref in ((0, keys_ref), (1, values_ref)):
                copy = pltpu.make_async_copy(
                    ref.at[block, 0, :, lanes],
                    outs[turn].at[slot, kind],
                    sems.at[turn * slots * 2 + slot * 2 + kind],
                )
                copy.start()
                copies.append(copy)
    for copy in copies:
        copy.wait()


def gather_requests(request, past_keys, past_values, count, slots, heads):
    block, width = past_keys.shape[2], past_keys.shape[3] // heads
    piece = jax.ShapeDtypeStruct((slots, 2, block, width), past_keys.dtype)
    return pl.pallas_call(
        functools.partial(gather_kernel, count, slots, heads, width),
        out_shape=[piece] * count,
        in_specs=[
            pl.BlockSpec(memory_space=pltpu.SMEM),
            pl.BlockSpec(memory_space=pltpu.VMEM),
            pl.BlockSpec(memory_space=pltpu.VMEM),
        ],
        out_specs=[pl.BlockSpec(memory_space=pl.ANY)] * count,
        scratch_shapes=[pltpu.SemaphoreType.DMA((count * slots * 2,))],
    )(request, past_keys, past_values)


def partial_attention(query_ref, keys, values, out_ref, stat_ref, group, mask):
    block, width = keys.shape
    factor = width**-0.5 * math.log2(math.e)
    values_t = values.T
    for member in range(group):
        query = query_ref[:, member * width : (member + 1) * width]
        span = slice(member * block, (member + 1) * block)
        scores = lax.dot_general(
            keys, query, (((1,), (1,)), ((), ())), preferred_element_type=jnp.float32
        )
        if mask is not None:
            scores = jnp.where(mask, scores, -jnp.inf)
        top = jnp.max(scores, axis=0, keepdims=True) * factor
        weights = jnp.exp2(scores * factor - top)
        stat_ref[0, 0:1, span] = top
        stat_ref[0, 1:2, span] = jnp.sum(weights, axis=0, keepdims=True)
        out_ref[0, :, span] = jnp.dot(
            values_t, weights.astype(jnp.bfloat16), preferred_element_type=jnp.float32
        ).astype(jnp.bfloat16)


def near_kernel(group, query_ref, keys_ref, values_ref, out_ref, stat_ref):
    block = keys_ref.shape[0]
    mask = lax.broadcasted_iota(jnp.int32, (block, block), 0) <= lax.broadcasted_iota(
        jnp.int32, (block, block), 1
    )
    partial_attention(
        query_ref, keys_ref[...], values_ref[...], out_ref, stat_ref, group, mask
    )


def far_kernel(group, rows_ref, query_ref, pair_ref, _out, _stat, out_ref, stat_ref):
    partial_attention(
        query_ref, pair_ref[0, 0], pair_ref[0, 1], out_ref, stat_ref, group, None
    )


def merge_kernel(group, picks, places_ref, *refs):
    outs, stats, result_ref = refs[: picks + 1], refs[picks + 1 : 2 * picks + 2], refs[-1]
    width = outs[0].shape[1]
    block = result_ref.shape[0]
    for member in range(group):
        span = slice(member * block, (member + 1) * block)
        tops = [stat[0, 0:1, span] for stat in stats]
        top = functools.reduce(jnp.maximum, tops)
        scales = [jnp.exp2(item - top) for item in tops]
        total = sum(scale * stat[0, 1:2, span] for scale, stat in zip(scales, stats))
        inverse = 1.0 / total
        mixed = sum(
            out[0, :, span].astype(jnp.float32) * (scale * inverse)
            for out, scale in zip(outs, scales)
        )
        result_ref[:, member * width : (member + 1) * width] = mixed.astype(jnp.bfloat16).T


def plain_shards(queries, span_keys, span_values, past_keys, past_values, selected):
    count = lax.axis_size("seq")
    me = lax.axis_index("seq")
    local_blocks, heads, picks = selected.shape
    needed = local_blocks * heads * picks
    rows = local_blocks * heads
    slots = (needed + count - 1) // count
    block = queries.shape[0] // local_blocks
    width = past_keys.shape[-1] // heads
    group = queries.shape[1] // (heads * width)
    span = group * block

    chosen = selected.reshape(-1)
    owners = chosen % count
    ranks = owner_ranks(owners)
    head_flat = lax.broadcasted_iota(jnp.int32, selected.shape, 1).reshape(-1)
    wanted = chosen // count * heads + head_flat
    slot_ids = owners * slots + ranks
    match = slot_ids[None, :] == jnp.arange(count * slots, dtype=jnp.int32)[:, None]
    outgoing = jnp.sum(jnp.where(match, wanted[None, :], 0), axis=1).reshape(count, slots)
    incoming = lax.all_to_all(outgoing, "seq", split_axis=0, concat_axis=0, tiled=True)

    turns = [0]
    for step in range(1, count // 2 + 1):
        turns.append(step)
        if step != count - step:
            turns.append(count - step)
    turns_array = jnp.array(turns, dtype=jnp.int32)
    request = jnp.take(incoming, (me + turns_array) % count, axis=0).reshape(-1)
    sources = (me - turns_array) % count
    place_ids = (sources[:, None] * slots + jnp.arange(slots, dtype=jnp.int32)).reshape(-1)
    found = place_ids[:, None] == slot_ids[None, :]
    pick_rows = jnp.arange(needed, dtype=jnp.int32) // picks
    pair_rows = jnp.sum(jnp.where(found, pick_rows[None, :], 0), axis=1).astype(jnp.int32)
    place_of = jnp.sum(
        jnp.where(found, jnp.arange(count * slots, dtype=jnp.int32)[:, None], 0), axis=0
    ).astype(jnp.int32)

    pieces = gather_requests(request, past_keys, past_values, count, slots, heads)
    arrived = [pieces[0]]
    for turn, piece in zip(turns[1:], pieces[1:]):
        arrived.append(
            lax.ppermute(piece, "seq", [(d, (d + turn) % count) for d in range(count)])
        )

    places = count * slots + rows
    partial_shapes = [
        jax.ShapeDtypeStruct((places, width, span), jnp.bfloat16),
        jax.ShapeDtypeStruct((places, 2, span), jnp.float32),
    ]
    pair_cost = 4 * span * block * width
    outs, stats = pl.pallas_call(
        functools.partial(near_kernel, group),
        grid=(rows,),
        in_specs=[
            pl.BlockSpec((block, group * width), lambda i: (i // heads, i % heads)),
            pl.BlockSpec((block, width), lambda i: (i // heads, i % heads)),
            pl.BlockSpec((block, width), lambda i: (i // heads, i % heads)),
        ],
        out_specs=[
            pl.BlockSpec((1, width, span), lambda i: (i + count * slots, 0, 0)),
            pl.BlockSpec((1, 2, span), lambda i: (i + count * slots, 0, 0)),
        ],
        out_shape=partial_shapes,
        cost_estimate=pl.CostEstimate(
            flops=rows * pair_cost, bytes_accessed=rows * 1500000, transcendentals=0
        ),
    )(queries, span_keys, span_values)

    size = max(count // GROUPS, 1)
    for first in range(0, count, size):
        pairs = jnp.concatenate(arrived[first : first + size], axis=0)
        length = pairs.shape[0]
        base = first * slots
        outs, stats = pl.pallas_call(
            functools.partial(far_kernel, group),
            grid_spec=pltpu.PrefetchScalarGridSpec(
                num_scalar_prefetch=1,
                grid=(length,),
                in_specs=[
                    pl.BlockSpec(
                        (block, group * width),
                        lambda i, r: (r[i] // heads, lax.rem(r[i], heads)),
                    ),
                    pl.BlockSpec((1, 2, block, width), lambda i, r: (i, 0, 0, 0)),
                    pl.BlockSpec(memory_space=pl.ANY),
                    pl.BlockSpec(memory_space=pl.ANY),
                ],
                out_specs=[
                    pl.BlockSpec((1, width, span), lambda i, r, base=base: (i + base, 0, 0)),
                    pl.BlockSpec((1, 2, span), lambda i, r, base=base: (i + base, 0, 0)),
                ],
            ),
            out_shape=partial_shapes,
            input_output_aliases={3: 0, 4: 1},
            cost_estimate=pl.CostEstimate(
                flops=length * pair_cost, bytes_accessed=length * 1500000, transcendentals=0
            ),
        )(lax.dynamic_slice_in_dim(pair_rows, base, length), queries, pairs, outs, stats)

    def far_place(pick):
        return lambda i, p: (p[i * picks + pick], 0, 0)

    maps = [far_place(pick) for pick in range(picks)]
    maps.append(lambda i, p: (i + count * slots, 0, 0))
    return pl.pallas_call(
        functools.partial(merge_kernel, group, picks),
        grid_spec=pltpu.PrefetchScalarGridSpec(
            num_scalar_prefetch=1,
            grid=(rows,),
            in_specs=[pl.BlockSpec((1, width, span), item) for item in maps]
            + [pl.BlockSpec((1, 2, span), item) for item in maps],
            out_specs=pl.BlockSpec(
                (block, group * width), lambda i, p: (i // heads, i % heads)
            ),
        ),
        out_shape=jax.ShapeDtypeStruct(queries.shape, queries.dtype),
    )(place_of, *([outs] * (picks + 1)), *([stats] * (picks + 1)))


MESH = pl.DeviceIdType.MESH
CHUNKS = 4
VMEM_BYTES = 65_000_000


def crossed(a, b, bits):
    total = 0
    for bit in range(bits):
        total = total + (a // 2**bit + b // 2**bit) % 2 * 2**bit
    return total


def attend(take_query, keys, values, store_out, store_stat, group, mask):
    block, width = keys.shape
    factor = width**-0.5 * math.log2(math.e)
    values_t = values.T
    for member in range(group):
        scores = lax.dot_general(
            keys,
            take_query(member),
            (((1,), (1,)), ((), ())),
            preferred_element_type=jnp.float32,
        )
        if mask is not None:
            scores = jnp.where(mask, scores, -jnp.inf)
        top = jnp.max(scores, axis=0, keepdims=True) * factor
        weights = jnp.exp2(scores * factor - top)
        store_stat(member, top, jnp.sum(weights, axis=0, keepdims=True))
        store_out(
            member,
            jnp.dot(
                values_t, weights.astype(jnp.bfloat16), preferred_element_type=jnp.float32
            ).astype(jnp.bfloat16),
        )


def exchange_kernel(
    heads,
    group,
    slots,
    ask_ref,
    rows_ref,
    queries_hbm,
    span_keys_hbm,
    span_values_hbm,
    past_keys_hbm,
    past_values_hbm,
    outs_hbm,
    stats_ref,
    query,
    near_keys,
    near_values,
    own,
    stage_own,
    stage_far,
    got_own,
    got_far,
    out_buf,
    told,
    told_scalar,
    *rest,
):
    mirror, sems = rest[:CHUNKS], rest[CHUNKS:]
    (load_sem, query_sem, out_sem, tell_send, tell_recv, tell_local, copy_send, copy_recv) = sems[:8]
    (own_send, own_recv, far_send, far_recv, whole_send, whole_recv) = sems[8:]
    count = lax.axis_size("seq")
    me = lax.axis_index("seq")
    half = ask_ref.shape[0]
    bits = half.bit_length() - 1
    middle = half // 2
    local = me % half
    base = me - local
    partner = (me + half) % count
    local_blocks = past_keys_hbm.shape[0]
    block, width = got_own.shape[-2:]
    part = block // CHUNKS
    rows = outs_hbm.shape[0] - count * slots

    def peer(turn):
        return base + crossed(local, turn, bits)

    def load_own(kind, head):
        source = (past_keys_hbm, past_values_hbm)[kind]
        lanes = pl.ds(pl.multiple_of(head * width, width), width)
        return pltpu.make_async_copy(
            source.at[:, 0, :, lanes], own.at[kind, :, head], load_sem.at[kind, head]
        )

    def load_near(kind, head):
        source, target = ((span_keys_hbm, near_keys), (span_values_hbm, near_values))[kind]
        lanes = pl.ds(pl.multiple_of(head * width, width), width)
        return pltpu.make_async_copy(
            source.at[:, :, lanes], target.at[head], load_sem.at[2 + kind, head]
        )

    def load_query(item):
        lanes = pl.ds(pl.multiple_of(item * width, width), width)
        return pltpu.make_async_copy(
            queries_hbm.at[:, :, lanes], query.at[item], query_sem.at[item]
        )

    def each_head(body):
        def step(head, carry):
            for kind in range(2):
                body(kind, head)
            return carry

        lax.fori_loop(0, heads, step, 0)

    def each_query(body):
        def step(item, carry):
            body(item)
            return carry

        lax.fori_loop(0, heads * group, step, 0)

    each_head(lambda kind, head: load_own(kind, head).start())
    each_head(lambda kind, head: load_near(kind, head).start())
    each_query(lambda item: load_query(item).start())

    barrier = pltpu.get_barrier_semaphore()

    def greet(turn, carry):
        pl.semaphore_signal(barrier, inc=1, device_id=(peer(turn),), device_id_type=MESH)
        return carry

    lax.fori_loop(1, half, greet, 0)
    pl.semaphore_signal(barrier, inc=1, device_id=(partner,), device_id_type=MESH)
    pl.semaphore_wait(barrier, half)

    def tell(turn):
        return pltpu.make_async_remote_copy(
            src_ref=ask_ref.at[turn],
            dst_ref=told.at[turn],
            send_sem=tell_send.at[turn],
            recv_sem=tell_recv.at[turn],
            device_id=(peer(turn),),
            device_id_type=MESH,
        )

    def mirror_copy(chunk, kind):
        return pltpu.make_async_remote_copy(
            src_ref=own.at[kind, :, :, pl.ds(chunk * part, part), :],
            dst_ref=mirror[chunk].at[kind],
            send_sem=copy_send.at[chunk * 2 + kind],
            recv_sem=copy_recv.at[chunk * 2 + kind],
            device_id=(partner,),
            device_id_type=MESH,
        )

    def send_own(turn):
        return pltpu.make_async_remote_copy(
            src_ref=stage_own.at[turn],
            dst_ref=got_own.at[turn],
            send_sem=own_send.at[turn],
            recv_sem=own_recv.at[turn],
            device_id=(peer(turn),),
            device_id_type=MESH,
        )

    def send_whole(turn):
        return pltpu.make_async_remote_copy(
            src_ref=stage_far.at[turn],
            dst_ref=got_far.at[turn],
            send_sem=whole_send.at[turn],
            recv_sem=whole_recv.at[turn],
            device_id=(peer(turn),),
            device_id_type=MESH,
        )

    def send_far(chunk, turn):
        span = pl.ds(chunk * part, part)
        return pltpu.make_async_remote_copy(
            src_ref=stage_far.at[turn, :, :, span, :],
            dst_ref=got_far.at[turn, :, :, span, :],
            send_sem=far_send.at[chunk, turn],
            recv_sem=far_recv.at[chunk, turn],
            device_id=(peer(turn),),
            device_id_type=MESH,
        )

    def each_turn(first, body, last=half):
        def step(turn, carry):
            body(turn)
            return carry

        lax.fori_loop(first, last, step, 0)

    each_turn(1, lambda turn: tell(turn).start())
    each_head(lambda kind, head: load_own(kind, head).wait())
    for chunk in range(CHUNKS):
        for kind in range(2):
            mirror_copy(chunk, kind).start()

    each_turn(1, lambda turn: tell(turn).wait_recv())
    own_row = pltpu.make_async_copy(ask_ref.at[0], told_scalar.at[0], tell_local.at[0])
    other_rows = pltpu.make_async_copy(
        told.at[pl.ds(1, half - 1)], told_scalar.at[pl.ds(1, half - 1)], tell_local.at[1]
    )
    own_row.start()
    other_rows.start()
    own_row.wait()
    other_rows.wait()
    def wanted(turn, slot):
        return told_scalar[turn, 0, slot], told_scalar[turn, 0, 2 * slots + slot]

    def gather_own(store, turn):
        for slot in range(slots):
            which, head = wanted(turn, slot)
            for kind in range(2):
                store[turn, slot, kind] = own[kind, which, head]

    def gather_far(chunk, store, turn):
        for slot in range(slots):
            which, head = wanted(turn, slots + slot)
            for kind in range(2):
                store[turn, slot, kind, pl.ds(chunk * part, part), :] = mirror[chunk][
                    kind, which, head
                ]

    gather_own(got_own, 0)
    each_turn(1, functools.partial(gather_own, stage_own))
    each_turn(1, lambda turn: send_own(turn).start())

    def put_out(place, buffer):
        return pltpu.make_async_copy(out_buf.at[buffer], outs_hbm.at[place], out_sem.at[buffer])

    def pair(place, buffer, first, head, query_block, keys, values, mask):
        if first is not False:
            pl.when(jnp.logical_not(first))(put_out(place, buffer).wait)
        else:
            put_out(place, buffer).wait()

        def take_query(member):
            return query[head * group + member, query_block]

        def store_out(member, value):
            out_buf[buffer, :, pl.ds(member * block, block)] = value

        def store_stat(member, top, total):
            stats_ref[place, 0:1, pl.ds(member * block, block)] = top
            stats_ref[place, 1:2, pl.ds(member * block, block)] = total

        attend(take_query, keys, values, store_out, store_stat, group, mask)
        put_out(place, buffer).start()

    each_head(lambda kind, head: load_near(kind, head).wait())
    each_query(lambda item: load_query(item).wait())
    mask = lax.broadcasted_iota(jnp.int32, (block, block), 0) <= lax.broadcasted_iota(
        jnp.int32, (block, block), 1
    )

    def near_step(item, carry):
        for buffer in range(2):
            row = item * 2 + buffer
            query_block, head = row // heads, row % heads
            pair(
                count * slots + row,
                buffer,
                item == 0,
                head,
                query_block,
                near_keys[head, query_block],
                near_values[head, query_block],
                mask,
            )
        return carry

    lax.fori_loop(0, rows // 2, near_step, 0)

    def far_pair(turn, extra, slot, store):
        place = turn * (2 * slots) + extra + slot
        pair(
            place,
            slot % 2,
            False,
            rows_ref[count * slots + place],
            rows_ref[place],
            store[turn, slot, 0],
            store[turn, slot, 1],
            None,
        )

    def forward(chunk):
        for kind in range(2):
            mirror_copy(chunk, kind).wait_recv()
        gather_far(chunk, got_far, 0)
        each_turn(1, functools.partial(gather_far, chunk, stage_far))
        each_turn(1, lambda turn: send_far(chunk, turn).start(), middle)
        if chunk == CHUNKS - 1:
            each_turn(middle, lambda turn: send_whole(turn).start())

    forward_at = (0, half // 2, 3 * half // 4)

    def own_step(turn, carry):
        for chunk, place in enumerate(forward_at):
            pl.when(turn == place)(functools.partial(forward, chunk))

        @pl.when(turn > 0)
        def _():
            send_own(turn).wait_recv()

        for slot in range(slots):
            far_pair(turn, 0, slot, got_own)
        return carry

    lax.fori_loop(0, half, own_step, 0)
    forward(CHUNKS - 1)

    def far_step(item, carry):
        turn = item % 2 * middle + item // 2

        @pl.when(turn >= middle)
        def _():
            send_whole(turn).wait_recv()

        @pl.when(jnp.logical_and(turn > 0, turn < middle))
        def _():
            for chunk in range(CHUNKS):
                send_far(chunk, turn).wait_recv()

        for slot in range(slots):
            far_pair(turn, slots, slot, got_far)
        return carry

    lax.fori_loop(0, half, far_step, 0)

    for buffer in range(2):
        put_out(buffer, buffer).wait()
    each_turn(1, lambda turn: tell(turn).wait_send())
    each_turn(1, lambda turn: send_own(turn).wait_send())
    for chunk in range(CHUNKS):
        for kind in range(2):
            mirror_copy(chunk, kind).wait_send()
        each_turn(1, lambda turn: send_far(chunk, turn).wait_send(), middle)
    each_turn(middle, lambda turn: send_whole(turn).wait_send())


def mirrored_shards(queries, span_keys, span_values, past_keys, past_values, selected):
    count = lax.axis_size("seq")
    me = lax.axis_index("seq")
    local_blocks, heads, picks = selected.shape
    needed = local_blocks * heads * picks
    rows = local_blocks * heads
    slots = needed // count
    half = count // 2
    block = queries.shape[0] // local_blocks
    width = past_keys.shape[-1] // heads
    group = queries.shape[1] // (heads * width)
    span = group * block
    kind = past_keys.dtype

    chosen = selected.reshape(-1)
    owners = chosen % count
    away = (owners // half != me // half).astype(jnp.int32)
    turns = (owners % half) ^ (me % half)
    places = turns * (2 * slots) + away * slots + owner_ranks(owners)
    found = jnp.arange(needed, dtype=jnp.int32)[:, None] == places[None, :]
    head_flat = lax.broadcasted_iota(jnp.int32, selected.shape, 1).reshape(-1)
    query_blocks = lax.broadcasted_iota(jnp.int32, selected.shape, 0).reshape(-1)

    def placed(values):
        return jnp.sum(jnp.where(found, values[None, :], 0), axis=1).astype(jnp.int32)

    place_heads = placed(head_flat)
    pair_rows = jnp.concatenate([placed(query_blocks), place_heads])
    ask = jnp.concatenate(
        [
            placed(chosen // count).reshape(half, 1, 2 * slots),
            place_heads.reshape(half, 1, 2 * slots),
            jnp.zeros((half, 1, 128 - 4 * slots), jnp.int32),
        ],
        axis=2,
    )

    total = count * slots + rows
    store = pltpu.VMEM((half, slots, 2, block, width), kind)
    dma = pltpu.SemaphoreType.DMA
    outs, stats = pl.pallas_call(
        functools.partial(exchange_kernel, heads, group, slots),
        in_specs=[
            pl.BlockSpec(memory_space=pltpu.VMEM),
            pl.BlockSpec(memory_space=pltpu.SMEM),
        ]
        + [pl.BlockSpec(memory_space=pl.ANY)] * 5,
        out_specs=[
            pl.BlockSpec(memory_space=pl.ANY),
            pl.BlockSpec(memory_space=pltpu.VMEM),
        ],
        out_shape=[
            jax.ShapeDtypeStruct((total, width, span), jnp.bfloat16),
            jax.ShapeDtypeStruct((total, 2, span), jnp.float32),
        ],
        scratch_shapes=[
            pltpu.VMEM((heads * group, local_blocks, block, width), queries.dtype),
            pltpu.VMEM((heads, local_blocks, block, width), span_keys.dtype),
            pltpu.VMEM((heads, local_blocks, block, width), span_values.dtype),
            pltpu.VMEM((2, past_keys.shape[0], heads, block, width), kind),
            store,
            store,
            store,
            store,
            pltpu.VMEM((2, width, span), jnp.bfloat16),
            pltpu.VMEM((half, 1, 128), jnp.int32),
            pltpu.SMEM((half, 1, 128), jnp.int32),
        ]
        + [pltpu.VMEM((2, past_keys.shape[0], heads, block // CHUNKS, width), kind)] * CHUNKS
        + [
            dma((4, heads)),
            dma((heads * group,)),
            dma((2,)),
            dma((half,)),
            dma((half,)),
            dma((2,)),
            dma((2 * CHUNKS,)),
            dma((2 * CHUNKS,)),
            dma((half,)),
            dma((half,)),
            dma((CHUNKS, half // 2)),
            dma((CHUNKS, half // 2)),
            dma((half,)),
            dma((half,)),
        ],
        compiler_params=pltpu.CompilerParams(
            collective_id=0, has_side_effects=True, vmem_limit_bytes=VMEM_BYTES
        ),
    )(
        ask,
        pair_rows,
        queries.reshape(local_blocks, block, -1),
        span_keys.reshape(local_blocks, block, -1),
        span_values.reshape(local_blocks, block, -1),
        past_keys,
        past_values,
    )

    def far_place(pick):
        return lambda i, p: (p[i * picks + pick], 0, 0)

    maps = [far_place(pick) for pick in range(picks)]
    maps.append(lambda i, p: (i + count * slots, 0, 0))
    return pl.pallas_call(
        functools.partial(merge_kernel, group, picks),
        grid_spec=pltpu.PrefetchScalarGridSpec(
            num_scalar_prefetch=1,
            grid=(rows,),
            in_specs=[pl.BlockSpec((1, width, span), item) for item in maps]
            + [pl.BlockSpec((1, 2, span), item) for item in maps],
            out_specs=pl.BlockSpec(
                (block, group * width), lambda i, p: (i // heads, i % heads)
            ),
        ),
        out_shape=jax.ShapeDtypeStruct(queries.shape, queries.dtype),
    )(places, *([outs] * (picks + 1)), *([stats] * (picks + 1)))


def shards(queries, span_keys, span_values, past_keys, past_values, selected):
    count = lax.axis_size("seq")
    needed = selected.size
    half = count // 2
    held = 2 * (queries.size + 2 * span_keys.size + 4 * past_keys.size)
    held += 16 * needed * past_keys.shape[2] * (past_keys.shape[3] // selected.shape[1]) // 2
    fits = held < VMEM_BYTES - 2**23
    whole = needed == count * max(needed // count, 1) and needed // max(count, 1) == 2
    if fits and whole and half >= 2 * CHUNKS and half & (half - 1) == 0:
        call = mirrored_shards
    else:
        call = plain_shards
    return call(queries, span_keys, span_values, past_keys, past_values, selected)


def solution(mesh):
    return jax.shard_map(
        shards,
        mesh=mesh,
        in_specs=(
            P("seq", None),
            P("seq", None),
            P("seq", None),
            P(None, "seq", None, None),
            P(None, "seq", None, None),
            P("seq", None, None),
        ),
        out_specs=P("seq", None),
        check_vma=False,
    )
```

```python
import functools
import math

import jax
import jax.numpy as jnp
from jax import lax
from jax.experimental import pallas as pl
from jax.experimental.pallas import tpu as pltpu
from jax.sharding import PartitionSpec as P


GROUPS = 8


def owner_ranks(owners):
    length = owners.shape[-1]
    later = lax.broadcasted_iota(jnp.int32, (length, length), 0)
    sooner = lax.broadcasted_iota(jnp.int32, (length, length), 1)
    same = owners[..., :, None] == owners[..., None, :]
    return jnp.sum(jnp.where(same & (sooner < later), 1, 0), axis=-1).astype(jnp.int32)


def gather_kernel(count, slots, heads, width, request_ref, keys_ref, values_ref, *rest):
    outs, sems = rest[:count], rest[count]
    copies = []
    for turn in range(count):
        for slot in range(slots):
            request = request_ref[turn * slots + slot]
            block, head = request // heads, lax.rem(request, heads)
            lanes = pl.ds(pl.multiple_of(head * width, width), width)
            for kind, ref in ((0, keys_ref), (1, values_ref)):
                copy = pltpu.make_async_copy(
                    ref.at[block, 0, :, lanes],
                    outs[turn].at[slot, kind],
                    sems.at[turn * slots * 2 + slot * 2 + kind],
                )
                copy.start()
                copies.append(copy)
    for copy in copies:
        copy.wait()


def gather_requests(request, past_keys, past_values, count, slots, heads):
    block, width = past_keys.shape[2], past_keys.shape[3] // heads
    piece = jax.ShapeDtypeStruct((slots, 2, block, width), past_keys.dtype)
    return pl.pallas_call(
        functools.partial(gather_kernel, count, slots, heads, width),
        out_shape=[piece] * count,
        in_specs=[
            pl.BlockSpec(memory_space=pltpu.SMEM),
            pl.BlockSpec(memory_space=pltpu.VMEM),
            pl.BlockSpec(memory_space=pltpu.VMEM),
        ],
        out_specs=[pl.BlockSpec(memory_space=pl.ANY)] * count,
        scratch_shapes=[pltpu.SemaphoreType.DMA((count * slots * 2,))],
    )(request, past_keys, past_values)


def partial_attention(query_ref, keys, values, out_ref, stat_ref, group, mask):
    block, width = keys.shape
    factor = width**-0.5 * math.log2(math.e)
    values_t = values.T
    for member in range(group):
        query = query_ref[:, member * width : (member + 1) * width]
        span = slice(member * block, (member + 1) * block)
        scores = lax.dot_general(
            keys, query, (((1,), (1,)), ((), ())), preferred_element_type=jnp.float32
        )
        if mask is not None:
            scores = jnp.where(mask, scores, -jnp.inf)
        top = jnp.max(scores, axis=0, keepdims=True) * factor
        weights = jnp.exp2(scores * factor - top)
        stat_ref[0, 0:1, span] = top
        stat_ref[0, 1:2, span] = jnp.sum(weights, axis=0, keepdims=True)
        out_ref[0, :, span] = jnp.dot(
            values_t, weights.astype(jnp.bfloat16), preferred_element_type=jnp.float32
        ).astype(jnp.bfloat16)


def near_kernel(group, query_ref, keys_ref, values_ref, out_ref, stat_ref):
    block = keys_ref.shape[0]
    mask = lax.broadcasted_iota(jnp.int32, (block, block), 0) <= lax.broadcasted_iota(
        jnp.int32, (block, block), 1
    )
    partial_attention(
        query_ref, keys_ref[...], values_ref[...], out_ref, stat_ref, group, mask
    )


def far_kernel(group, rows_ref, query_ref, pair_ref, _out, _stat, out_ref, stat_ref):
    partial_attention(
        query_ref, pair_ref[0, 0], pair_ref[0, 1], out_ref, stat_ref, group, None
    )


def merge_kernel(group, picks, places_ref, *refs):
    outs, stats, result_ref = refs[: picks + 1], refs[picks + 1 : 2 * picks + 2], refs[-1]
    width = outs[0].shape[1]
    block = result_ref.shape[0]
    for member in range(group):
        span = slice(member * block, (member + 1) * block)
        tops = [stat[0, 0:1, span] for stat in stats]
        top = functools.reduce(jnp.maximum, tops)
        scales = [jnp.exp2(item - top) for item in tops]
        total = sum(scale * stat[0, 1:2, span] for scale, stat in zip(scales, stats))
        inverse = 1.0 / total
        mixed = sum(
            out[0, :, span].astype(jnp.float32) * (scale * inverse)
            for out, scale in zip(outs, scales)
        )
        result_ref[:, member * width : (member + 1) * width] = mixed.astype(jnp.bfloat16).T


def plain_shards(queries, span_keys, span_values, past_keys, past_values, selected):
    count = lax.axis_size("seq")
    me = lax.axis_index("seq")
    local_blocks, heads, picks = selected.shape
    needed = local_blocks * heads * picks
    rows = local_blocks * heads
    slots = (needed + count - 1) // count
    block = queries.shape[0] // local_blocks
    width = past_keys.shape[-1] // heads
    group = queries.shape[1] // (heads * width)
    span = group * block

    chosen = selected.reshape(-1)
    owners = chosen % count
    ranks = owner_ranks(owners)
    head_flat = lax.broadcasted_iota(jnp.int32, selected.shape, 1).reshape(-1)
    wanted = chosen // count * heads + head_flat
    slot_ids = owners * slots + ranks
    match = slot_ids[None, :] == jnp.arange(count * slots, dtype=jnp.int32)[:, None]
    outgoing = jnp.sum(jnp.where(match, wanted[None, :], 0), axis=1).reshape(count, slots)
    incoming = lax.all_to_all(outgoing, "seq", split_axis=0, concat_axis=0, tiled=True)

    turns = [0]
    for step in range(1, count // 2 + 1):
        turns.append(step)
        if step != count - step:
            turns.append(count - step)
    turns_array = jnp.array(turns, dtype=jnp.int32)
    request = jnp.take(incoming, (me + turns_array) % count, axis=0).reshape(-1)
    sources = (me - turns_array) % count
    place_ids = (sources[:, None] * slots + jnp.arange(slots, dtype=jnp.int32)).reshape(-1)
    found = place_ids[:, None] == slot_ids[None, :]
    pick_rows = jnp.arange(needed, dtype=jnp.int32) // picks
    pair_rows = jnp.sum(jnp.where(found, pick_rows[None, :], 0), axis=1).astype(jnp.int32)
    place_of = jnp.sum(
        jnp.where(found, jnp.arange(count * slots, dtype=jnp.int32)[:, None], 0), axis=0
    ).astype(jnp.int32)

    pieces = gather_requests(request, past_keys, past_values, count, slots, heads)
    arrived = [pieces[0]]
    for turn, piece in zip(turns[1:], pieces[1:]):
        arrived.append(
            lax.ppermute(piece, "seq", [(d, (d + turn) % count) for d in range(count)])
        )

    places = count * slots + rows
    partial_shapes = [
        jax.ShapeDtypeStruct((places, width, span), jnp.bfloat16),
        jax.ShapeDtypeStruct((places, 2, span), jnp.float32),
    ]
    pair_cost = 4 * span * block * width
    outs, stats = pl.pallas_call(
        functools.partial(near_kernel, group),
        grid=(rows,),
        in_specs=[
            pl.BlockSpec((block, group * width), lambda i: (i // heads, i % heads)),
            pl.BlockSpec((block, width), lambda i: (i // heads, i % heads)),
            pl.BlockSpec((block, width), lambda i: (i // heads, i % heads)),
        ],
        out_specs=[
            pl.BlockSpec((1, width, span), lambda i: (i + count * slots, 0, 0)),
            pl.BlockSpec((1, 2, span), lambda i: (i + count * slots, 0, 0)),
        ],
        out_shape=partial_shapes,
        cost_estimate=pl.CostEstimate(
            flops=rows * pair_cost, bytes_accessed=rows * 1500000, transcendentals=0
        ),
    )(queries, span_keys, span_values)

    size = max(count // GROUPS, 1)
    for first in range(0, count, size):
        pairs = jnp.concatenate(arrived[first : first + size], axis=0)
        length = pairs.shape[0]
        base = first * slots
        outs, stats = pl.pallas_call(
            functools.partial(far_kernel, group),
            grid_spec=pltpu.PrefetchScalarGridSpec(
                num_scalar_prefetch=1,
                grid=(length,),
                in_specs=[
                    pl.BlockSpec(
                        (block, group * width),
                        lambda i, r: (r[i] // heads, lax.rem(r[i], heads)),
                    ),
                    pl.BlockSpec((1, 2, block, width), lambda i, r: (i, 0, 0, 0)),
                    pl.BlockSpec(memory_space=pl.ANY),
                    pl.BlockSpec(memory_space=pl.ANY),
                ],
                out_specs=[
                    pl.BlockSpec((1, width, span), lambda i, r, base=base: (i + base, 0, 0)),
                    pl.BlockSpec((1, 2, span), lambda i, r, base=base: (i + base, 0, 0)),
                ],
            ),
            out_shape=partial_shapes,
            input_output_aliases={3: 0, 4: 1},
            cost_estimate=pl.CostEstimate(
                flops=length * pair_cost, bytes_accessed=length * 1500000, transcendentals=0
            ),
        )(lax.dynamic_slice_in_dim(pair_rows, base, length), queries, pairs, outs, stats)

    def far_place(pick):
        return lambda i, p: (p[i * picks + pick], 0, 0)

    maps = [far_place(pick) for pick in range(picks)]
    maps.append(lambda i, p: (i + count * slots, 0, 0))
    return pl.pallas_call(
        functools.partial(merge_kernel, group, picks),
        grid_spec=pltpu.PrefetchScalarGridSpec(
            num_scalar_prefetch=1,
            grid=(rows,),
            in_specs=[pl.BlockSpec((1, width, span), item) for item in maps]
            + [pl.BlockSpec((1, 2, span), item) for item in maps],
            out_specs=pl.BlockSpec(
                (block, group * width), lambda i, p: (i // heads, i % heads)
            ),
        ),
        out_shape=jax.ShapeDtypeStruct(queries.shape, queries.dtype),
    )(place_of, *([outs] * (picks + 1)), *([stats] * (picks + 1)))


MESH = pl.DeviceIdType.MESH
CHUNKS = 4
VMEM_BYTES = 65_000_000


def crossed(a, b, bits):
    total = 0
    for bit in range(bits):
        total = total + (a // 2**bit + b // 2**bit) % 2 * 2**bit
    return total


def turn_orders(half):
    middle = half // 2
    straight = [middle, middle + 1]

    def hops(turn):
        return (turn // 2).bit_count()

    queues = []
    for first_link in (2, 0):
        turns = [t for t in range(2, half) if t & 2 == first_link and t not in straight]
        outer = sorted(
            (t for t in turns if t >= middle), key=lambda t: (hops(t), t % 2, -t)
        )
        inner = sorted((t for t in turns if t < middle), key=lambda t: (t % 2, hops(t), t))
        queue = [t for both in zip(outer, inner) for t in both]
        queue += outer[len(inner) :] + inner[len(outer) :]
        queues += [((2 * i + 1) / len(queue), turn) for i, turn in enumerate(queue)]
    turned = [turn for _, turn in sorted(queues)]
    late = sorted(
        range(middle, half), key=lambda t: (hops(t) > 2, t % 2, hops(t), -t)
    )
    return straight, turned + [1], [0, 1] + straight + turned, list(range(middle)) + late


def listed(item, values):
    result = values[-1]
    for index, value in enumerate(values[:-1]):
        result = jnp.where(item == index, value, result)
    return result


def attend(take_query, keys, values, store_out, store_stat, group, mask):
    block, width = keys.shape
    factor = width**-0.5 * math.log2(math.e)
    values_t = values.T
    for member in range(group):
        scores = lax.dot_general(
            keys,
            take_query(member),
            (((1,), (1,)), ((), ())),
            preferred_element_type=jnp.float32,
        )
        if mask is not None:
            scores = jnp.where(mask, scores, -jnp.inf)
        top = jnp.max(scores, axis=0, keepdims=True) * factor
        weights = jnp.exp2(scores * factor - top)
        store_stat(member, top, jnp.sum(weights, axis=0, keepdims=True))
        store_out(
            member,
            jnp.dot(
                values_t, weights.astype(jnp.bfloat16), preferred_element_type=jnp.float32
            ).astype(jnp.bfloat16),
        )


def exchange_kernel(
    heads,
    group,
    slots,
    ask_ref,
    rows_ref,
    queries_hbm,
    span_keys_hbm,
    span_values_hbm,
    past_keys_hbm,
    past_values_hbm,
    outs_hbm,
    stats_ref,
    query,
    near_keys,
    near_values,
    own,
    stage_own,
    stage_far,
    got_own,
    got_far,
    out_buf,
    told,
    told_scalar,
    *rest,
):
    mirror, sems = rest[:CHUNKS], rest[CHUNKS:]
    (load_sem, query_sem, out_sem, tell_send, tell_recv, tell_local, copy_send, copy_recv) = sems[:8]
    (own_send, own_recv, far_send, far_recv, whole_send, whole_recv) = sems[8:]
    count = lax.axis_size("seq")
    me = lax.axis_index("seq")
    half = ask_ref.shape[0]
    bits = half.bit_length() - 1
    middle = half // 2
    straight, turned, own_order, far_order = turn_orders(half)
    forward_at = (half // 8, 3 * half // 8, 9 * half // 16, 3 * half // 4)
    local = me % half
    base = me - local
    partner = (me + half) % count
    local_blocks = past_keys_hbm.shape[0]
    block, width = got_own.shape[-2:]
    part = block // CHUNKS
    rows = outs_hbm.shape[0] - count * slots

    def peer(turn):
        return base + crossed(local, turn, bits)

    def load_own(kind, head):
        source = (past_keys_hbm, past_values_hbm)[kind]
        lanes = pl.ds(pl.multiple_of(head * width, width), width)
        return pltpu.make_async_copy(
            source.at[:, 0, :, lanes], own.at[kind, :, head], load_sem.at[kind, head]
        )

    def load_near(kind, head):
        source, target = ((span_keys_hbm, near_keys), (span_values_hbm, near_values))[kind]
        lanes = pl.ds(pl.multiple_of(head * width, width), width)
        return pltpu.make_async_copy(
            source.at[:, :, lanes], target.at[head], load_sem.at[2 + kind, head]
        )

    def load_query(item):
        lanes = pl.ds(pl.multiple_of(item * width, width), width)
        return pltpu.make_async_copy(
            queries_hbm.at[:, :, lanes], query.at[item], query_sem.at[item]
        )

    def each_head(body):
        def step(head, carry):
            for kind in range(2):
                body(kind, head)
            return carry

        lax.fori_loop(0, heads, step, 0)

    def each_query(body):
        def step(item, carry):
            body(item)
            return carry

        lax.fori_loop(0, heads * group, step, 0)

    each_head(lambda kind, head: load_own(kind, head).start())
    each_head(lambda kind, head: load_near(kind, head).start())
    each_query(lambda item: load_query(item).start())

    barrier = pltpu.get_barrier_semaphore()

    def greet(turn, carry):
        pl.semaphore_signal(barrier, inc=1, device_id=(peer(turn),), device_id_type=MESH)
        return carry

    lax.fori_loop(1, half, greet, 0)
    pl.semaphore_signal(barrier, inc=1, device_id=(partner,), device_id_type=MESH)
    pl.semaphore_wait(barrier, half)

    def tell(turn):
        return pltpu.make_async_remote_copy(
            src_ref=ask_ref.at[turn],
            dst_ref=told.at[turn],
            send_sem=tell_send.at[turn],
            recv_sem=tell_recv.at[turn],
            device_id=(peer(turn),),
            device_id_type=MESH,
        )

    def mirror_copy(chunk, kind):
        return pltpu.make_async_remote_copy(
            src_ref=own.at[kind, :, :, pl.ds(chunk * part, part), :],
            dst_ref=mirror[chunk].at[kind],
            send_sem=copy_send.at[chunk * 2 + kind],
            recv_sem=copy_recv.at[chunk * 2 + kind],
            device_id=(partner,),
            device_id_type=MESH,
        )

    def send_own(turn):
        return pltpu.make_async_remote_copy(
            src_ref=stage_own.at[turn],
            dst_ref=got_own.at[turn],
            send_sem=own_send.at[turn],
            recv_sem=own_recv.at[turn],
            device_id=(peer(turn),),
            device_id_type=MESH,
        )

    def send_whole(turn):
        return pltpu.make_async_remote_copy(
            src_ref=stage_far.at[turn],
            dst_ref=got_far.at[turn],
            send_sem=whole_send.at[turn],
            recv_sem=whole_recv.at[turn],
            device_id=(peer(turn),),
            device_id_type=MESH,
        )

    def send_far(chunk, turn):
        span = pl.ds(chunk * part, part)
        return pltpu.make_async_remote_copy(
            src_ref=stage_far.at[turn, :, :, span, :],
            dst_ref=got_far.at[turn, :, :, span, :],
            send_sem=far_send.at[chunk, turn],
            recv_sem=far_recv.at[chunk, turn],
            device_id=(peer(turn),),
            device_id_type=MESH,
        )

    def each_turn(first, body, last=half):
        def step(turn, carry):
            body(turn)
            return carry

        lax.fori_loop(first, last, step, 0)

    each_turn(1, lambda turn: tell(turn).start())
    each_head(lambda kind, head: load_own(kind, head).wait())
    def start_mirror(chunk):
        for kind in range(2):
            mirror_copy(chunk, kind).start()

    start_mirror(0)

    each_turn(1, lambda turn: tell(turn).wait_recv())
    own_row = pltpu.make_async_copy(ask_ref.at[0], told_scalar.at[0], tell_local.at[0])
    other_rows = pltpu.make_async_copy(
        told.at[pl.ds(1, half - 1)], told_scalar.at[pl.ds(1, half - 1)], tell_local.at[1]
    )
    own_row.start()
    other_rows.start()
    own_row.wait()
    other_rows.wait()
    def wanted(turn, slot):
        return told_scalar[turn, 0, slot], told_scalar[turn, 0, 2 * slots + slot]

    def gather_own(store, turn):
        for slot in range(slots):
            which, head = wanted(turn, slot)
            for kind in range(2):
                store[turn, slot, kind] = own[kind, which, head]

    def gather_far(chunk, store, turn):
        for slot in range(slots):
            which, head = wanted(turn, slots + slot)
            for kind in range(2):
                store[turn, slot, kind, pl.ds(chunk * part, part), :] = mirror[chunk][
                    kind, which, head
                ]

    gather_own(got_own, 0)
    each_turn(1, functools.partial(gather_own, stage_own))
    for turn in straight:
        send_own(turn).start()
    for chunk in range(1, CHUNKS):
        start_mirror(chunk)
    for turn in turned:
        send_own(turn).start()

    def put_out(place, buffer):
        return pltpu.make_async_copy(out_buf.at[buffer], outs_hbm.at[place], out_sem.at[buffer])

    def pair(place, buffer, first, head, query_block, keys, values, mask):
        if first is not False:
            pl.when(jnp.logical_not(first))(put_out(place, buffer).wait)
        else:
            put_out(place, buffer).wait()

        def take_query(member):
            return query[head * group + member, query_block]

        def store_out(member, value):
            out_buf[buffer, :, pl.ds(member * block, block)] = value

        def store_stat(member, top, total):
            stats_ref[place, 0:1, pl.ds(member * block, block)] = top
            stats_ref[place, 1:2, pl.ds(member * block, block)] = total

        attend(take_query, keys, values, store_out, store_stat, group, mask)
        put_out(place, buffer).start()

    each_head(lambda kind, head: load_near(kind, head).wait())
    each_query(lambda item: load_query(item).wait())
    mask = lax.broadcasted_iota(jnp.int32, (block, block), 0) <= lax.broadcasted_iota(
        jnp.int32, (block, block), 1
    )

    def near_step(item, carry):
        for buffer in range(2):
            row = item * 2 + buffer
            query_block, head = row // heads, row % heads
            pair(
                count * slots + row,
                buffer,
                item == 0,
                head,
                query_block,
                near_keys[head, query_block],
                near_values[head, query_block],
                mask,
            )
        return carry

    lax.fori_loop(0, rows // 2, near_step, 0)

    def far_pair(turn, extra, slot, store):
        place = turn * (2 * slots) + extra + slot
        pair(
            place,
            slot % 2,
            False,
            rows_ref[count * slots + place],
            rows_ref[place],
            store[turn, slot, 0],
            store[turn, slot, 1],
            None,
        )

    def forward(chunk):
        for kind in range(2):
            mirror_copy(chunk, kind).wait_recv()
        gather_far(chunk, got_far, 0)
        each_turn(1, functools.partial(gather_far, chunk, stage_far))
        each_turn(1, lambda turn: send_far(chunk, turn).start(), middle)
        if chunk == CHUNKS - 1:
            each_turn(middle, lambda turn: send_whole(turn).start())

    def own_step(item, carry):
        for chunk, place in enumerate(forward_at):
            pl.when(item == place)(functools.partial(forward, chunk))
        turn = listed(item, own_order)

        @pl.when(turn > 0)
        def _():
            send_own(turn).wait_recv()

        for slot in range(slots):
            far_pair(turn, 0, slot, got_own)
        return carry

    lax.fori_loop(0, half, own_step, 0)

    def far_step(item, carry):
        turn = listed(item, far_order)

        @pl.when(turn >= middle)
        def _():
            send_whole(turn).wait_recv()

        @pl.when(jnp.logical_and(turn > 0, turn < middle))
        def _():
            for chunk in range(CHUNKS):
                send_far(chunk, turn).wait_recv()

        for slot in range(slots):
            far_pair(turn, slots, slot, got_far)
        return carry

    lax.fori_loop(0, half, far_step, 0)

    for buffer in range(2):
        put_out(buffer, buffer).wait()
    each_turn(1, lambda turn: tell(turn).wait_send())
    each_turn(1, lambda turn: send_own(turn).wait_send())
    for chunk in range(CHUNKS):
        for kind in range(2):
            mirror_copy(chunk, kind).wait_send()
        each_turn(1, lambda turn: send_far(chunk, turn).wait_send(), middle)
    each_turn(middle, lambda turn: send_whole(turn).wait_send())


def mirrored_shards(queries, span_keys, span_values, past_keys, past_values, selected):
    count = lax.axis_size("seq")
    me = lax.axis_index("seq")
    local_blocks, heads, picks = selected.shape
    needed = local_blocks * heads * picks
    rows = local_blocks * heads
    slots = needed // count
    half = count // 2
    block = queries.shape[0] // local_blocks
    width = past_keys.shape[-1] // heads
    group = queries.shape[1] // (heads * width)
    span = group * block
    kind = past_keys.dtype

    chosen = selected.reshape(-1)
    owners = chosen % count
    away = (owners // half != me // half).astype(jnp.int32)
    turns = (owners % half) ^ (me % half)
    places = turns * (2 * slots) + away * slots + owner_ranks(owners)
    found = jnp.arange(needed, dtype=jnp.int32)[:, None] == places[None, :]
    head_flat = lax.broadcasted_iota(jnp.int32, selected.shape, 1).reshape(-1)
    query_blocks = lax.broadcasted_iota(jnp.int32, selected.shape, 0).reshape(-1)

    def placed(values):
        return jnp.sum(jnp.where(found, values[None, :], 0), axis=1).astype(jnp.int32)

    place_heads = placed(head_flat)
    pair_rows = jnp.concatenate([placed(query_blocks), place_heads])
    ask = jnp.concatenate(
        [
            placed(chosen // count).reshape(half, 1, 2 * slots),
            place_heads.reshape(half, 1, 2 * slots),
            jnp.zeros((half, 1, 128 - 4 * slots), jnp.int32),
        ],
        axis=2,
    )

    total = count * slots + rows
    store = pltpu.VMEM((half, slots, 2, block, width), kind)
    dma = pltpu.SemaphoreType.DMA
    outs, stats = pl.pallas_call(
        functools.partial(exchange_kernel, heads, group, slots),
        in_specs=[
            pl.BlockSpec(memory_space=pltpu.VMEM),
            pl.BlockSpec(memory_space=pltpu.SMEM),
        ]
        + [pl.BlockSpec(memory_space=pl.ANY)] * 5,
        out_specs=[
            pl.BlockSpec(memory_space=pl.ANY),
            pl.BlockSpec(memory_space=pltpu.VMEM),
        ],
        out_shape=[
            jax.ShapeDtypeStruct((total, width, span), jnp.bfloat16),
            jax.ShapeDtypeStruct((total, 2, span), jnp.float32),
        ],
        scratch_shapes=[
            pltpu.VMEM((heads * group, local_blocks, block, width), queries.dtype),
            pltpu.VMEM((heads, local_blocks, block, width), span_keys.dtype),
            pltpu.VMEM((heads, local_blocks, block, width), span_values.dtype),
            pltpu.VMEM((2, past_keys.shape[0], heads, block, width), kind),
            store,
            store,
            store,
            store,
            pltpu.VMEM((2, width, span), jnp.bfloat16),
            pltpu.VMEM((half, 1, 128), jnp.int32),
            pltpu.SMEM((half, 1, 128), jnp.int32),
        ]
        + [pltpu.VMEM((2, past_keys.shape[0], heads, block // CHUNKS, width), kind)] * CHUNKS
        + [
            dma((4, heads)),
            dma((heads * group,)),
            dma((2,)),
            dma((half,)),
            dma((half,)),
            dma((2,)),
            dma((2 * CHUNKS,)),
            dma((2 * CHUNKS,)),
            dma((half,)),
            dma((half,)),
            dma((CHUNKS, half // 2)),
            dma((CHUNKS, half // 2)),
            dma((half,)),
            dma((half,)),
        ],
        compiler_params=pltpu.CompilerParams(
            collective_id=0, has_side_effects=True, vmem_limit_bytes=VMEM_BYTES
        ),
    )(
        ask,
        pair_rows,
        queries.reshape(local_blocks, block, -1),
        span_keys.reshape(local_blocks, block, -1),
        span_values.reshape(local_blocks, block, -1),
        past_keys,
        past_values,
    )

    def far_place(pick):
        return lambda i, p: (p[i * picks + pick], 0, 0)

    maps = [far_place(pick) for pick in range(picks)]
    maps.append(lambda i, p: (i + count * slots, 0, 0))
    return pl.pallas_call(
        functools.partial(merge_kernel, group, picks),
        grid_spec=pltpu.PrefetchScalarGridSpec(
            num_scalar_prefetch=1,
            grid=(rows,),
            in_specs=[pl.BlockSpec((1, width, span), item) for item in maps]
            + [pl.BlockSpec((1, 2, span), item) for item in maps],
            out_specs=pl.BlockSpec(
                (block, group * width), lambda i, p: (i // heads, i % heads)
            ),
        ),
        out_shape=jax.ShapeDtypeStruct(queries.shape, queries.dtype),
    )(places, *([outs] * (picks + 1)), *([stats] * (picks + 1)))


def shards(queries, span_keys, span_values, past_keys, past_values, selected):
    count = lax.axis_size("seq")
    needed = selected.size
    half = count // 2
    held = 2 * (queries.size + 2 * span_keys.size + 4 * past_keys.size)
    held += 16 * needed * past_keys.shape[2] * (past_keys.shape[3] // selected.shape[1]) // 2
    fits = held < VMEM_BYTES - 2**23
    whole = needed == count * max(needed // count, 1) and needed // max(count, 1) == 2
    if fits and whole and half >= 2 * CHUNKS and half & (half - 1) == 0:
        call = mirrored_shards
    else:
        call = plain_shards
    return call(queries, span_keys, span_values, past_keys, past_values, selected)


def solution(mesh):
    return jax.shard_map(
        shards,
        mesh=mesh,
        in_specs=(
            P("seq", None),
            P("seq", None),
            P("seq", None),
            P(None, "seq", None, None),
            P(None, "seq", None, None),
            P("seq", None, None),
        ),
        out_specs=P("seq", None),
        check_vma=False,
    )
```

```python
import functools
import math

import jax
import jax.numpy as jnp
from jax import lax
from jax.experimental import pallas as pl
from jax.experimental.pallas import tpu as pltpu
from jax.sharding import PartitionSpec as P


GROUPS = 8


def owner_ranks(owners):
    length = owners.shape[-1]
    later = lax.broadcasted_iota(jnp.int32, (length, length), 0)
    sooner = lax.broadcasted_iota(jnp.int32, (length, length), 1)
    same = owners[..., :, None] == owners[..., None, :]
    return jnp.sum(jnp.where(same & (sooner < later), 1, 0), axis=-1).astype(jnp.int32)


def gather_kernel(count, slots, heads, width, request_ref, keys_ref, values_ref, *rest):
    outs, sems = rest[:count], rest[count]
    copies = []
    for turn in range(count):
        for slot in range(slots):
            request = request_ref[turn * slots + slot]
            block, head = request // heads, lax.rem(request, heads)
            lanes = pl.ds(pl.multiple_of(head * width, width), width)
            for kind, ref in ((0, keys_ref), (1, values_ref)):
                copy = pltpu.make_async_copy(
                    ref.at[block, 0, :, lanes],
                    outs[turn].at[slot, kind],
                    sems.at[turn * slots * 2 + slot * 2 + kind],
                )
                copy.start()
                copies.append(copy)
    for copy in copies:
        copy.wait()


def gather_requests(request, past_keys, past_values, count, slots, heads):
    block, width = past_keys.shape[2], past_keys.shape[3] // heads
    piece = jax.ShapeDtypeStruct((slots, 2, block, width), past_keys.dtype)
    return pl.pallas_call(
        functools.partial(gather_kernel, count, slots, heads, width),
        out_shape=[piece] * count,
        in_specs=[
            pl.BlockSpec(memory_space=pltpu.SMEM),
            pl.BlockSpec(memory_space=pltpu.VMEM),
            pl.BlockSpec(memory_space=pltpu.VMEM),
        ],
        out_specs=[pl.BlockSpec(memory_space=pl.ANY)] * count,
        scratch_shapes=[pltpu.SemaphoreType.DMA((count * slots * 2,))],
    )(request, past_keys, past_values)


def partial_attention(query_ref, keys, values, out_ref, stat_ref, group, mask):
    block, width = keys.shape
    factor = width**-0.5 * math.log2(math.e)
    values_t = values.T
    for member in range(group):
        query = query_ref[:, member * width : (member + 1) * width]
        span = slice(member * block, (member + 1) * block)
        scores = lax.dot_general(
            keys, query, (((1,), (1,)), ((), ())), preferred_element_type=jnp.float32
        )
        if mask is not None:
            scores = jnp.where(mask, scores, -jnp.inf)
        top = jnp.max(scores, axis=0, keepdims=True) * factor
        weights = jnp.exp2(scores * factor - top)
        stat_ref[0, 0:1, span] = top
        stat_ref[0, 1:2, span] = jnp.sum(weights, axis=0, keepdims=True)
        out_ref[0, :, span] = jnp.dot(
            values_t, weights.astype(jnp.bfloat16), preferred_element_type=jnp.float32
        ).astype(jnp.bfloat16)


def near_kernel(group, query_ref, keys_ref, values_ref, out_ref, stat_ref):
    block = keys_ref.shape[0]
    mask = lax.broadcasted_iota(jnp.int32, (block, block), 0) <= lax.broadcasted_iota(
        jnp.int32, (block, block), 1
    )
    partial_attention(
        query_ref, keys_ref[...], values_ref[...], out_ref, stat_ref, group, mask
    )


def far_kernel(group, rows_ref, query_ref, pair_ref, _out, _stat, out_ref, stat_ref):
    partial_attention(
        query_ref, pair_ref[0, 0], pair_ref[0, 1], out_ref, stat_ref, group, None
    )


def merge_kernel(group, picks, places_ref, *refs):
    outs, stats, result_ref = refs[: picks + 1], refs[picks + 1 : 2 * picks + 2], refs[-1]
    width = outs[0].shape[1]
    block = result_ref.shape[0]
    for member in range(group):
        span = slice(member * block, (member + 1) * block)
        tops = [stat[0, 0:1, span] for stat in stats]
        top = functools.reduce(jnp.maximum, tops)
        scales = [jnp.exp2(item - top) for item in tops]
        total = sum(scale * stat[0, 1:2, span] for scale, stat in zip(scales, stats))
        inverse = 1.0 / total
        mixed = sum(
            out[0, :, span].astype(jnp.float32) * (scale * inverse)
            for out, scale in zip(outs, scales)
        )
        result_ref[:, member * width : (member + 1) * width] = mixed.astype(jnp.bfloat16).T


def plain_shards(queries, span_keys, span_values, past_keys, past_values, selected):
    count = lax.axis_size("seq")
    me = lax.axis_index("seq")
    local_blocks, heads, picks = selected.shape
    needed = local_blocks * heads * picks
    rows = local_blocks * heads
    slots = (needed + count - 1) // count
    block = queries.shape[0] // local_blocks
    width = past_keys.shape[-1] // heads
    group = queries.shape[1] // (heads * width)
    span = group * block

    chosen = selected.reshape(-1)
    owners = chosen % count
    ranks = owner_ranks(owners)
    head_flat = lax.broadcasted_iota(jnp.int32, selected.shape, 1).reshape(-1)
    wanted = chosen // count * heads + head_flat
    slot_ids = owners * slots + ranks
    match = slot_ids[None, :] == jnp.arange(count * slots, dtype=jnp.int32)[:, None]
    outgoing = jnp.sum(jnp.where(match, wanted[None, :], 0), axis=1).reshape(count, slots)
    incoming = lax.all_to_all(outgoing, "seq", split_axis=0, concat_axis=0, tiled=True)

    turns = [0]
    for step in range(1, count // 2 + 1):
        turns.append(step)
        if step != count - step:
            turns.append(count - step)
    turns_array = jnp.array(turns, dtype=jnp.int32)
    request = jnp.take(incoming, (me + turns_array) % count, axis=0).reshape(-1)
    sources = (me - turns_array) % count
    place_ids = (sources[:, None] * slots + jnp.arange(slots, dtype=jnp.int32)).reshape(-1)
    found = place_ids[:, None] == slot_ids[None, :]
    pick_rows = jnp.arange(needed, dtype=jnp.int32) // picks
    pair_rows = jnp.sum(jnp.where(found, pick_rows[None, :], 0), axis=1).astype(jnp.int32)
    place_of = jnp.sum(
        jnp.where(found, jnp.arange(count * slots, dtype=jnp.int32)[:, None], 0), axis=0
    ).astype(jnp.int32)

    pieces = gather_requests(request, past_keys, past_values, count, slots, heads)
    arrived = [pieces[0]]
    for turn, piece in zip(turns[1:], pieces[1:]):
        arrived.append(
            lax.ppermute(piece, "seq", [(d, (d + turn) % count) for d in range(count)])
        )

    places = count * slots + rows
    partial_shapes = [
        jax.ShapeDtypeStruct((places, width, span), jnp.bfloat16),
        jax.ShapeDtypeStruct((places, 2, span), jnp.float32),
    ]
    pair_cost = 4 * span * block * width
    outs, stats = pl.pallas_call(
        functools.partial(near_kernel, group),
        grid=(rows,),
        in_specs=[
            pl.BlockSpec((block, group * width), lambda i: (i // heads, i % heads)),
            pl.BlockSpec((block, width), lambda i: (i // heads, i % heads)),
            pl.BlockSpec((block, width), lambda i: (i // heads, i % heads)),
        ],
        out_specs=[
            pl.BlockSpec((1, width, span), lambda i: (i + count * slots, 0, 0)),
            pl.BlockSpec((1, 2, span), lambda i: (i + count * slots, 0, 0)),
        ],
        out_shape=partial_shapes,
        cost_estimate=pl.CostEstimate(
            flops=rows * pair_cost, bytes_accessed=rows * 1500000, transcendentals=0
        ),
    )(queries, span_keys, span_values)

    size = max(count // GROUPS, 1)
    for first in range(0, count, size):
        pairs = jnp.concatenate(arrived[first : first + size], axis=0)
        length = pairs.shape[0]
        base = first * slots
        outs, stats = pl.pallas_call(
            functools.partial(far_kernel, group),
            grid_spec=pltpu.PrefetchScalarGridSpec(
                num_scalar_prefetch=1,
                grid=(length,),
                in_specs=[
                    pl.BlockSpec(
                        (block, group * width),
                        lambda i, r: (r[i] // heads, lax.rem(r[i], heads)),
                    ),
                    pl.BlockSpec((1, 2, block, width), lambda i, r: (i, 0, 0, 0)),
                    pl.BlockSpec(memory_space=pl.ANY),
                    pl.BlockSpec(memory_space=pl.ANY),
                ],
                out_specs=[
                    pl.BlockSpec((1, width, span), lambda i, r, base=base: (i + base, 0, 0)),
                    pl.BlockSpec((1, 2, span), lambda i, r, base=base: (i + base, 0, 0)),
                ],
            ),
            out_shape=partial_shapes,
            input_output_aliases={3: 0, 4: 1},
            cost_estimate=pl.CostEstimate(
                flops=length * pair_cost, bytes_accessed=length * 1500000, transcendentals=0
            ),
        )(lax.dynamic_slice_in_dim(pair_rows, base, length), queries, pairs, outs, stats)

    def far_place(pick):
        return lambda i, p: (p[i * picks + pick], 0, 0)

    maps = [far_place(pick) for pick in range(picks)]
    maps.append(lambda i, p: (i + count * slots, 0, 0))
    return pl.pallas_call(
        functools.partial(merge_kernel, group, picks),
        grid_spec=pltpu.PrefetchScalarGridSpec(
            num_scalar_prefetch=1,
            grid=(rows,),
            in_specs=[pl.BlockSpec((1, width, span), item) for item in maps]
            + [pl.BlockSpec((1, 2, span), item) for item in maps],
            out_specs=pl.BlockSpec(
                (block, group * width), lambda i, p: (i // heads, i % heads)
            ),
        ),
        out_shape=jax.ShapeDtypeStruct(queries.shape, queries.dtype),
    )(place_of, *([outs] * (picks + 1)), *([stats] * (picks + 1)))


MESH = pl.DeviceIdType.MESH
CHUNKS = 4
RING = 4
VMEM_BYTES = 65_000_000


def crossed(a, b, bits):
    total = 0
    for bit in range(bits):
        total = total + (a // 2**bit + b // 2**bit) % 2 * 2**bit
    return total


def turn_orders(half):
    middle = half // 2
    straight = [middle, middle + 1]

    def hops(turn):
        return (turn // 2).bit_count()

    queues = []
    for first_link in (2, 0):
        turns = [t for t in range(2, half) if t & 2 == first_link and t not in straight]
        outer = sorted(
            (t for t in turns if t >= middle), key=lambda t: (hops(t), t % 2, -t)
        )
        inner = sorted((t for t in turns if t < middle), key=lambda t: (t % 2, hops(t), t))
        queue = [t for both in zip(outer, inner) for t in both]
        queue += outer[len(inner) :] + inner[len(outer) :]
        queues += [((2 * i + 1) / len(queue), turn) for i, turn in enumerate(queue)]
    turned = [turn for _, turn in sorted(queues)]
    late = sorted(
        range(middle, half), key=lambda t: (hops(t) > 2, t % 2, hops(t), -t)
    )
    return straight, turned + [1], [0, 1] + straight + turned, list(range(middle)) + late


def listed(item, values):
    result = values[-1]
    for index, value in enumerate(values[:-1]):
        result = jnp.where(item == index, value, result)
    return result


def attend(take_query, keys, values, store_out, store_stat, group, mask):
    block, width = keys.shape
    factor = width**-0.5 * math.log2(math.e)
    values_t = values.T
    for member in range(group):
        scores = lax.dot_general(
            keys,
            take_query(member),
            (((1,), (1,)), ((), ())),
            preferred_element_type=jnp.float32,
        )
        if mask is not None:
            scores = jnp.where(mask, scores, -jnp.inf)
        top = jnp.max(scores, axis=0, keepdims=True) * factor
        weights = jnp.exp2(scores * factor - top)
        store_stat(member, top, jnp.sum(weights, axis=0, keepdims=True))
        store_out(
            member,
            jnp.dot(
                values_t, weights.astype(jnp.bfloat16), preferred_element_type=jnp.float32
            ).astype(jnp.bfloat16),
        )


def exchange_kernel(
    heads,
    group,
    slots,
    ask_ref,
    rows_ref,
    queries_hbm,
    span_keys_hbm,
    span_values_hbm,
    past_keys_hbm,
    past_values_hbm,
    outs_hbm,
    stats_ref,
    query,
    near_keys,
    near_values,
    own,
    stage_own,
    stage_far,
    got_own,
    got_far,
    out_buf,
    told,
    told_scalar,
    *rest,
):
    mirror, sems = rest[:CHUNKS], rest[CHUNKS:]
    (load_sem, query_sem, out_sem, tell_send, tell_recv, tell_local, copy_send, copy_recv) = sems[:8]
    (own_send, own_recv, far_send, far_recv, whole_send, whole_recv) = sems[8:]
    count = lax.axis_size("seq")
    me = lax.axis_index("seq")
    half = ask_ref.shape[0]
    bits = half.bit_length() - 1
    middle = half // 2
    straight, turned, own_order, far_order = turn_orders(half)
    forward_at = (half // 8, 3 * half // 8, 9 * half // 16, 3 * half // 4)
    local = me % half
    base = me - local
    partner = (me + half) % count
    local_blocks = past_keys_hbm.shape[0]
    block, width = got_own.shape[-2:]
    part = block // CHUNKS
    rows = outs_hbm.shape[0] - count * slots

    def peer(turn):
        return base + crossed(local, turn, bits)

    def load_own(kind, head):
        source = (past_keys_hbm, past_values_hbm)[kind]
        lanes = pl.ds(pl.multiple_of(head * width, width), width)
        return pltpu.make_async_copy(
            source.at[:, 0, :, lanes], own.at[kind, :, head], load_sem.at[kind, head]
        )

    def load_near(kind, head):
        source, target = ((span_keys_hbm, near_keys), (span_values_hbm, near_values))[kind]
        lanes = pl.ds(pl.multiple_of(head * width, width), width)
        return pltpu.make_async_copy(
            source.at[:, :, lanes], target.at[head], load_sem.at[2 + kind, head]
        )

    def load_query(item):
        lanes = pl.ds(pl.multiple_of(item * width, width), width)
        return pltpu.make_async_copy(
            queries_hbm.at[:, :, lanes], query.at[item], query_sem.at[item]
        )

    def each_head(body):
        def step(head, carry):
            for kind in range(2):
                body(kind, head)
            return carry

        lax.fori_loop(0, heads, step, 0)

    def each_query(body):
        def step(item, carry):
            body(item)
            return carry

        lax.fori_loop(0, heads * group, step, 0)

    each_head(lambda kind, head: load_own(kind, head).start())
    each_head(lambda kind, head: load_near(kind, head).start())
    each_query(lambda item: load_query(item).start())

    barrier = pltpu.get_barrier_semaphore()

    def greet(turn, carry):
        pl.semaphore_signal(barrier, inc=1, device_id=(peer(turn),), device_id_type=MESH)
        return carry

    lax.fori_loop(1, half, greet, 0)
    pl.semaphore_signal(barrier, inc=1, device_id=(partner,), device_id_type=MESH)
    pl.semaphore_wait(barrier, half)

    def tell(turn):
        return pltpu.make_async_remote_copy(
            src_ref=ask_ref.at[turn],
            dst_ref=told.at[turn],
            send_sem=tell_send.at[turn],
            recv_sem=tell_recv.at[turn],
            device_id=(peer(turn),),
            device_id_type=MESH,
        )

    def mirror_copy(chunk, kind):
        return pltpu.make_async_remote_copy(
            src_ref=own.at[kind, :, :, pl.ds(chunk * part, part), :],
            dst_ref=mirror[chunk].at[kind],
            send_sem=copy_send.at[chunk * 2 + kind],
            recv_sem=copy_recv.at[chunk * 2 + kind],
            device_id=(partner,),
            device_id_type=MESH,
        )

    def send_own(turn):
        return pltpu.make_async_remote_copy(
            src_ref=stage_own.at[turn],
            dst_ref=got_own.at[turn],
            send_sem=own_send.at[turn],
            recv_sem=own_recv.at[turn],
            device_id=(peer(turn),),
            device_id_type=MESH,
        )

    def send_whole(turn, slot):
        return pltpu.make_async_remote_copy(
            src_ref=stage_far.at[turn, slot],
            dst_ref=got_far.at[turn, slot],
            send_sem=whole_send.at[turn, slot],
            recv_sem=whole_recv.at[turn, slot],
            device_id=(peer(turn),),
            device_id_type=MESH,
        )

    def send_far(chunk, turn):
        span = pl.ds(chunk * part, part)
        return pltpu.make_async_remote_copy(
            src_ref=stage_far.at[turn, :, :, span, :],
            dst_ref=got_far.at[turn, :, :, span, :],
            send_sem=far_send.at[chunk, turn],
            recv_sem=far_recv.at[chunk, turn],
            device_id=(peer(turn),),
            device_id_type=MESH,
        )

    def each_slot(body):
        def both(turn):
            for slot in range(slots):
                body(turn, slot)

        return both

    def each_turn(first, body, last=half):
        def step(turn, carry):
            body(turn)
            return carry

        lax.fori_loop(first, last, step, 0)

    each_turn(1, lambda turn: tell(turn).start())
    each_head(lambda kind, head: load_own(kind, head).wait())
    def start_mirror(chunk):
        for kind in range(2):
            mirror_copy(chunk, kind).start()

    start_mirror(0)

    each_turn(1, lambda turn: tell(turn).wait_recv())
    own_row = pltpu.make_async_copy(ask_ref.at[0], told_scalar.at[0], tell_local.at[0])
    other_rows = pltpu.make_async_copy(
        told.at[pl.ds(1, half - 1)], told_scalar.at[pl.ds(1, half - 1)], tell_local.at[1]
    )
    own_row.start()
    other_rows.start()
    own_row.wait()
    other_rows.wait()
    def wanted(turn, slot):
        return told_scalar[turn, 0, slot], told_scalar[turn, 0, 2 * slots + slot]

    def gather_own(store, turn):
        for slot in range(slots):
            which, head = wanted(turn, slot)
            for kind in range(2):
                store[turn, slot, kind] = own[kind, which, head]

    def gather_far(chunk, store, turn):
        for slot in range(slots):
            which, head = wanted(turn, slots + slot)
            for kind in range(2):
                store[turn, slot, kind, pl.ds(chunk * part, part), :] = mirror[chunk][
                    kind, which, head
                ]

    gather_own(got_own, 0)
    each_turn(1, functools.partial(gather_own, stage_own))
    for turn in straight:
        send_own(turn).start()
    for chunk in range(1, CHUNKS):
        start_mirror(chunk)
    for turn in turned:
        send_own(turn).start()

    def put_out(place, buffer):
        return pltpu.make_async_copy(out_buf.at[buffer], outs_hbm.at[place], out_sem.at[buffer])

    def pair(place, buffer, first, head, query_block, keys, values, mask):
        if first is not False:
            pl.when(jnp.logical_not(first))(put_out(place, buffer).wait)
        else:
            put_out(place, buffer).wait()

        def take_query(member):
            return query[head * group + member, query_block]

        def store_out(member, value):
            out_buf[buffer, :, pl.ds(member * block, block)] = value

        def store_stat(member, top, total):
            stats_ref[place, 0:1, pl.ds(member * block, block)] = top
            stats_ref[place, 1:2, pl.ds(member * block, block)] = total

        attend(take_query, keys, values, store_out, store_stat, group, mask)
        put_out(place, buffer).start()

    each_head(lambda kind, head: load_near(kind, head).wait())
    each_query(lambda item: load_query(item).wait())
    mask = lax.broadcasted_iota(jnp.int32, (block, block), 0) <= lax.broadcasted_iota(
        jnp.int32, (block, block), 1
    )

    def near_step(item, carry):
        for buffer in range(2):
            row = item * 2 + buffer
            query_block, head = row // heads, row % heads
            pair(
                count * slots + row,
                buffer,
                item == 0,
                head,
                query_block,
                near_keys[head, query_block],
                near_values[head, query_block],
                mask,
            )
        return carry

    lax.fori_loop(0, rows // 2, near_step, 0)

    def far_pair(turn, extra, slot, store):
        place = turn * (2 * slots) + extra + slot
        pair(
            place,
            slot % 2,
            False,
            rows_ref[count * slots + place],
            rows_ref[place],
            store[turn, slot, 0],
            store[turn, slot, 1],
            None,
        )

    def forward(chunk):
        for kind in range(2):
            mirror_copy(chunk, kind).wait_recv()
        gather_far(chunk, got_far, 0)
        each_turn(1, functools.partial(gather_far, chunk, stage_far))
        each_turn(1, lambda turn: send_far(chunk, turn).start(), middle)
        if chunk == CHUNKS - 1:
            each_turn(middle, each_slot(lambda turn, slot: send_whole(turn, slot).start()))

    def own_step(item, carry):
        for chunk, place in enumerate(forward_at):
            pl.when(item == place)(functools.partial(forward, chunk))
        turn = listed(item, own_order)

        @pl.when(turn > 0)
        def _():
            send_own(turn).wait_recv()

        for slot in range(slots):
            far_pair(turn, 0, slot, got_own)
        return carry

    lax.fori_loop(0, half, own_step, 0)

    def far_step(item, carry):
        turn = listed(item, far_order)

        @pl.when(jnp.logical_and(turn > 0, turn < middle))
        def _():
            for chunk in range(CHUNKS):
                send_far(chunk, turn).wait_recv()

        for slot in range(slots):
            pl.when(turn >= middle)(send_whole(turn, slot).wait_recv)
            far_pair(turn, slots, slot, got_far)
        return carry

    lax.fori_loop(0, half, far_step, 0)

    for buffer in range(2):
        put_out(buffer, buffer).wait()
    each_turn(1, lambda turn: tell(turn).wait_send())
    each_turn(1, lambda turn: send_own(turn).wait_send())
    for chunk in range(CHUNKS):
        for kind in range(2):
            mirror_copy(chunk, kind).wait_send()
        each_turn(1, lambda turn: send_far(chunk, turn).wait_send(), middle)
    each_turn(middle, each_slot(lambda turn, slot: send_whole(turn, slot).wait_send()))


def join_kernel(
    group, picks, near_place, heads, places_ref, outs_hbm, stats, result_hbm, ring, made, in_sem, out_sem
):
    width, block = outs_hbm.shape[1], outs_hbm.shape[2] // group
    depth = ring.shape[0]
    rows = outs_hbm.shape[0] - near_place

    def places_of(row):
        return [places_ref[row * picks + pick] for pick in range(picks)] + [near_place + row]

    def fetches(row):
        slot = row % depth
        return [
            pltpu.make_async_copy(
                outs_hbm.at[place], ring.at[slot, item], in_sem.at[slot, item]
            )
            for item, place in enumerate(places_of(row))
        ]

    def put(row):
        lanes = pl.ds(pl.multiple_of(row % heads * (group * width), width), group * width)
        lines = pl.ds(pl.multiple_of(row // heads * block, block), block)
        return pltpu.make_async_copy(
            made.at[row % 2], result_hbm.at[lines, lanes], out_sem.at[row % 2]
        )

    def start(row):
        for copy in fetches(row):
            copy.start()

    for row in range(depth - 1):
        start(row)

    def step(row, carry):
        pl.when(row + depth - 1 < rows)(lambda: start(row + depth - 1))
        for copy in fetches(row):
            copy.wait()
        pl.when(row >= 2)(lambda: put(row - 2).wait())
        stat_places = places_of(row)
        for member in range(group):
            span = pl.ds(member * block, block)
            tops = [stats[place, 0:1, span] for place in stat_places]
            top = functools.reduce(jnp.maximum, tops)
            scales = [jnp.exp2(one - top) for one in tops]
            total = sum(
                scale * stats[place, 1:2, span] for scale, place in zip(scales, stat_places)
            )
            inverse = 1.0 / total
            mixed = sum(
                ring[row % depth, item, :, span].astype(jnp.float32) * (scale * inverse)
                for item, scale in enumerate(scales)
            )
            made[row % 2, :, pl.ds(member * width, width)] = mixed.astype(jnp.bfloat16).T
        put(row).start()
        return carry

    lax.fori_loop(0, rows, step, 0)
    for row in (rows - 2, rows - 1):
        put(row).wait()


def mirrored_shards(queries, span_keys, span_values, past_keys, past_values, selected):
    count = lax.axis_size("seq")
    me = lax.axis_index("seq")
    local_blocks, heads, picks = selected.shape
    needed = local_blocks * heads * picks
    rows = local_blocks * heads
    slots = needed // count
    half = count // 2
    block = queries.shape[0] // local_blocks
    width = past_keys.shape[-1] // heads
    group = queries.shape[1] // (heads * width)
    span = group * block
    kind = past_keys.dtype

    chosen = selected.reshape(-1)
    owners = chosen % count
    away = (owners // half != me // half).astype(jnp.int32)
    turns = (owners % half) ^ (me % half)
    places = turns * (2 * slots) + away * slots + owner_ranks(owners)
    found = jnp.arange(needed, dtype=jnp.int32)[:, None] == places[None, :]
    head_flat = lax.broadcasted_iota(jnp.int32, selected.shape, 1).reshape(-1)
    query_blocks = lax.broadcasted_iota(jnp.int32, selected.shape, 0).reshape(-1)

    def placed(values):
        return jnp.sum(jnp.where(found, values[None, :], 0), axis=1).astype(jnp.int32)

    place_heads = placed(head_flat)
    pair_rows = jnp.concatenate([placed(query_blocks), place_heads])
    ask = jnp.concatenate(
        [
            placed(chosen // count).reshape(half, 1, 2 * slots),
            place_heads.reshape(half, 1, 2 * slots),
            jnp.zeros((half, 1, 128 - 4 * slots), jnp.int32),
        ],
        axis=2,
    )

    total = count * slots + rows
    store = pltpu.VMEM((half, slots, 2, block, width), kind)
    dma = pltpu.SemaphoreType.DMA
    outs, stats = pl.pallas_call(
        functools.partial(exchange_kernel, heads, group, slots),
        in_specs=[
            pl.BlockSpec(memory_space=pltpu.VMEM),
            pl.BlockSpec(memory_space=pltpu.SMEM),
        ]
        + [pl.BlockSpec(memory_space=pl.ANY)] * 5,
        out_specs=[
            pl.BlockSpec(memory_space=pl.ANY),
            pl.BlockSpec(memory_space=pltpu.VMEM),
        ],
        out_shape=[
            jax.ShapeDtypeStruct((total, width, span), jnp.bfloat16),
            jax.ShapeDtypeStruct((total, 2, span), jnp.float32),
        ],
        scratch_shapes=[
            pltpu.VMEM((heads * group, local_blocks, block, width), queries.dtype),
            pltpu.VMEM((heads, local_blocks, block, width), span_keys.dtype),
            pltpu.VMEM((heads, local_blocks, block, width), span_values.dtype),
            pltpu.VMEM((2, past_keys.shape[0], heads, block, width), kind),
            store,
            store,
            store,
            store,
            pltpu.VMEM((2, width, span), jnp.bfloat16),
            pltpu.VMEM((half, 1, 128), jnp.int32),
            pltpu.SMEM((half, 1, 128), jnp.int32),
        ]
        + [pltpu.VMEM((2, past_keys.shape[0], heads, block // CHUNKS, width), kind)] * CHUNKS
        + [
            dma((4, heads)),
            dma((heads * group,)),
            dma((2,)),
            dma((half,)),
            dma((half,)),
            dma((2,)),
            dma((2 * CHUNKS,)),
            dma((2 * CHUNKS,)),
            dma((half,)),
            dma((half,)),
            dma((CHUNKS, half // 2)),
            dma((CHUNKS, half // 2)),
            dma((half, slots)),
            dma((half, slots)),
        ],
        compiler_params=pltpu.CompilerParams(
            collective_id=0, has_side_effects=True, vmem_limit_bytes=VMEM_BYTES
        ),
    )(
        ask,
        pair_rows,
        queries.reshape(local_blocks, block, -1),
        span_keys.reshape(local_blocks, block, -1),
        span_values.reshape(local_blocks, block, -1),
        past_keys,
        past_values,
    )

    return pl.pallas_call(
        functools.partial(join_kernel, group, picks, count * slots, heads),
        in_specs=[
            pl.BlockSpec(memory_space=pltpu.SMEM),
            pl.BlockSpec(memory_space=pl.ANY),
            pl.BlockSpec(memory_space=pltpu.VMEM),
        ],
        out_specs=pl.BlockSpec(memory_space=pl.ANY),
        out_shape=jax.ShapeDtypeStruct(queries.shape, queries.dtype),
        scratch_shapes=[
            pltpu.VMEM((RING, picks + 1, width, span), jnp.bfloat16),
            pltpu.VMEM((2, block, group * width), jnp.bfloat16),
            dma((RING, picks + 1)),
            dma((2,)),
        ],
        compiler_params=pltpu.CompilerParams(vmem_limit_bytes=VMEM_BYTES),
    )(places, outs, stats)


def shards(queries, span_keys, span_values, past_keys, past_values, selected):
    count = lax.axis_size("seq")
    needed = selected.size
    half = count // 2
    held = 2 * (queries.size + 2 * span_keys.size + 4 * past_keys.size)
    held += 16 * needed * past_keys.shape[2] * (past_keys.shape[3] // selected.shape[1]) // 2
    fits = held < VMEM_BYTES - 2**23
    whole = needed == count * max(needed // count, 1) and needed // max(count, 1) == 2
    if fits and whole and half >= 2 * CHUNKS and half & (half - 1) == 0:
        call = mirrored_shards
    else:
        call = plain_shards
    return call(queries, span_keys, span_values, past_keys, past_values, selected)


def solution(mesh):
    return jax.shard_map(
        shards,
        mesh=mesh,
        in_specs=(
            P("seq", None),
            P("seq", None),
            P("seq", None),
            P(None, "seq", None, None),
            P(None, "seq", None, None),
            P("seq", None, None),
        ),
        out_specs=P("seq", None),
        check_vma=False,
    )
```

```python
import functools
import math

import jax
import jax.numpy as jnp
from jax import lax
from jax.experimental import pallas as pl
from jax.experimental.pallas import tpu as pltpu
from jax.sharding import PartitionSpec as P


GROUPS = 8


def owner_ranks(owners):
    length = owners.shape[-1]
    later = lax.broadcasted_iota(jnp.int32, (length, length), 0)
    sooner = lax.broadcasted_iota(jnp.int32, (length, length), 1)
    same = owners[..., :, None] == owners[..., None, :]
    return jnp.sum(jnp.where(same & (sooner < later), 1, 0), axis=-1).astype(jnp.int32)


def gather_kernel(count, slots, heads, width, request_ref, keys_ref, values_ref, *rest):
    outs, sems = rest[:count], rest[count]
    copies = []
    for turn in range(count):
        for slot in range(slots):
            request = request_ref[turn * slots + slot]
            block, head = request // heads, lax.rem(request, heads)
            lanes = pl.ds(pl.multiple_of(head * width, width), width)
            for kind, ref in ((0, keys_ref), (1, values_ref)):
                copy = pltpu.make_async_copy(
                    ref.at[block, 0, :, lanes],
                    outs[turn].at[slot, kind],
                    sems.at[turn * slots * 2 + slot * 2 + kind],
                )
                copy.start()
                copies.append(copy)
    for copy in copies:
        copy.wait()


def gather_requests(request, past_keys, past_values, count, slots, heads):
    block, width = past_keys.shape[2], past_keys.shape[3] // heads
    piece = jax.ShapeDtypeStruct((slots, 2, block, width), past_keys.dtype)
    return pl.pallas_call(
        functools.partial(gather_kernel, count, slots, heads, width),
        out_shape=[piece] * count,
        in_specs=[
            pl.BlockSpec(memory_space=pltpu.SMEM),
            pl.BlockSpec(memory_space=pltpu.VMEM),
            pl.BlockSpec(memory_space=pltpu.VMEM),
        ],
        out_specs=[pl.BlockSpec(memory_space=pl.ANY)] * count,
        scratch_shapes=[pltpu.SemaphoreType.DMA((count * slots * 2,))],
    )(request, past_keys, past_values)


def partial_attention(query_ref, keys, values, out_ref, stat_ref, group, mask):
    block, width = keys.shape
    factor = width**-0.5 * math.log2(math.e)
    values_t = values.T
    for member in range(group):
        query = query_ref[:, member * width : (member + 1) * width]
        span = slice(member * block, (member + 1) * block)
        scores = lax.dot_general(
            keys, query, (((1,), (1,)), ((), ())), preferred_element_type=jnp.float32
        )
        if mask is not None:
            scores = jnp.where(mask, scores, -jnp.inf)
        top = jnp.max(scores, axis=0, keepdims=True) * factor
        weights = jnp.exp2(scores * factor - top)
        stat_ref[0, 0:1, span] = top
        stat_ref[0, 1:2, span] = jnp.sum(weights, axis=0, keepdims=True)
        out_ref[0, :, span] = jnp.dot(
            values_t, weights.astype(jnp.bfloat16), preferred_element_type=jnp.float32
        ).astype(jnp.bfloat16)


def near_kernel(group, query_ref, keys_ref, values_ref, out_ref, stat_ref):
    block = keys_ref.shape[0]
    mask = lax.broadcasted_iota(jnp.int32, (block, block), 0) <= lax.broadcasted_iota(
        jnp.int32, (block, block), 1
    )
    partial_attention(
        query_ref, keys_ref[...], values_ref[...], out_ref, stat_ref, group, mask
    )


def far_kernel(group, rows_ref, query_ref, pair_ref, _out, _stat, out_ref, stat_ref):
    partial_attention(
        query_ref, pair_ref[0, 0], pair_ref[0, 1], out_ref, stat_ref, group, None
    )


def merge_kernel(group, picks, places_ref, *refs):
    outs, stats, result_ref = refs[: picks + 1], refs[picks + 1 : 2 * picks + 2], refs[-1]
    width = outs[0].shape[1]
    block = result_ref.shape[0]
    for member in range(group):
        span = slice(member * block, (member + 1) * block)
        tops = [stat[0, 0:1, span] for stat in stats]
        top = functools.reduce(jnp.maximum, tops)
        scales = [jnp.exp2(item - top) for item in tops]
        total = sum(scale * stat[0, 1:2, span] for scale, stat in zip(scales, stats))
        inverse = 1.0 / total
        mixed = sum(
            out[0, :, span].astype(jnp.float32) * (scale * inverse)
            for out, scale in zip(outs, scales)
        )
        result_ref[:, member * width : (member + 1) * width] = mixed.astype(jnp.bfloat16).T


def plain_shards(queries, span_keys, span_values, past_keys, past_values, selected):
    count = lax.axis_size("seq")
    me = lax.axis_index("seq")
    local_blocks, heads, picks = selected.shape
    needed = local_blocks * heads * picks
    rows = local_blocks * heads
    slots = (needed + count - 1) // count
    block = queries.shape[0] // local_blocks
    width = past_keys.shape[-1] // heads
    group = queries.shape[1] // (heads * width)
    span = group * block

    chosen = selected.reshape(-1)
    owners = chosen % count
    ranks = owner_ranks(owners)
    head_flat = lax.broadcasted_iota(jnp.int32, selected.shape, 1).reshape(-1)
    wanted = chosen // count * heads + head_flat
    slot_ids = owners * slots + ranks
    match = slot_ids[None, :] == jnp.arange(count * slots, dtype=jnp.int32)[:, None]
    outgoing = jnp.sum(jnp.where(match, wanted[None, :], 0), axis=1).reshape(count, slots)
    incoming = lax.all_to_all(outgoing, "seq", split_axis=0, concat_axis=0, tiled=True)

    turns = [0]
    for step in range(1, count // 2 + 1):
        turns.append(step)
        if step != count - step:
            turns.append(count - step)
    turns_array = jnp.array(turns, dtype=jnp.int32)
    request = jnp.take(incoming, (me + turns_array) % count, axis=0).reshape(-1)
    sources = (me - turns_array) % count
    place_ids = (sources[:, None] * slots + jnp.arange(slots, dtype=jnp.int32)).reshape(-1)
    found = place_ids[:, None] == slot_ids[None, :]
    pick_rows = jnp.arange(needed, dtype=jnp.int32) // picks
    pair_rows = jnp.sum(jnp.where(found, pick_rows[None, :], 0), axis=1).astype(jnp.int32)
    place_of = jnp.sum(
        jnp.where(found, jnp.arange(count * slots, dtype=jnp.int32)[:, None], 0), axis=0
    ).astype(jnp.int32)

    pieces = gather_requests(request, past_keys, past_values, count, slots, heads)
    arrived = [pieces[0]]
    for turn, piece in zip(turns[1:], pieces[1:]):
        arrived.append(
            lax.ppermute(piece, "seq", [(d, (d + turn) % count) for d in range(count)])
        )

    places = count * slots + rows
    partial_shapes = [
        jax.ShapeDtypeStruct((places, width, span), jnp.bfloat16),
        jax.ShapeDtypeStruct((places, 2, span), jnp.float32),
    ]
    pair_cost = 4 * span * block * width
    outs, stats = pl.pallas_call(
        functools.partial(near_kernel, group),
        grid=(rows,),
        in_specs=[
            pl.BlockSpec((block, group * width), lambda i: (i // heads, i % heads)),
            pl.BlockSpec((block, width), lambda i: (i // heads, i % heads)),
            pl.BlockSpec((block, width), lambda i: (i // heads, i % heads)),
        ],
        out_specs=[
            pl.BlockSpec((1, width, span), lambda i: (i + count * slots, 0, 0)),
            pl.BlockSpec((1, 2, span), lambda i: (i + count * slots, 0, 0)),
        ],
        out_shape=partial_shapes,
        cost_estimate=pl.CostEstimate(
            flops=rows * pair_cost, bytes_accessed=rows * 1500000, transcendentals=0
        ),
    )(queries, span_keys, span_values)

    size = max(count // GROUPS, 1)
    for first in range(0, count, size):
        pairs = jnp.concatenate(arrived[first : first + size], axis=0)
        length = pairs.shape[0]
        base = first * slots
        outs, stats = pl.pallas_call(
            functools.partial(far_kernel, group),
            grid_spec=pltpu.PrefetchScalarGridSpec(
                num_scalar_prefetch=1,
                grid=(length,),
                in_specs=[
                    pl.BlockSpec(
                        (block, group * width),
                        lambda i, r: (r[i] // heads, lax.rem(r[i], heads)),
                    ),
                    pl.BlockSpec((1, 2, block, width), lambda i, r: (i, 0, 0, 0)),
                    pl.BlockSpec(memory_space=pl.ANY),
                    pl.BlockSpec(memory_space=pl.ANY),
                ],
                out_specs=[
                    pl.BlockSpec((1, width, span), lambda i, r, base=base: (i + base, 0, 0)),
                    pl.BlockSpec((1, 2, span), lambda i, r, base=base: (i + base, 0, 0)),
                ],
            ),
            out_shape=partial_shapes,
            input_output_aliases={3: 0, 4: 1},
            cost_estimate=pl.CostEstimate(
                flops=length * pair_cost, bytes_accessed=length * 1500000, transcendentals=0
            ),
        )(lax.dynamic_slice_in_dim(pair_rows, base, length), queries, pairs, outs, stats)

    def far_place(pick):
        return lambda i, p: (p[i * picks + pick], 0, 0)

    maps = [far_place(pick) for pick in range(picks)]
    maps.append(lambda i, p: (i + count * slots, 0, 0))
    return pl.pallas_call(
        functools.partial(merge_kernel, group, picks),
        grid_spec=pltpu.PrefetchScalarGridSpec(
            num_scalar_prefetch=1,
            grid=(rows,),
            in_specs=[pl.BlockSpec((1, width, span), item) for item in maps]
            + [pl.BlockSpec((1, 2, span), item) for item in maps],
            out_specs=pl.BlockSpec(
                (block, group * width), lambda i, p: (i // heads, i % heads)
            ),
        ),
        out_shape=jax.ShapeDtypeStruct(queries.shape, queries.dtype),
    )(place_of, *([outs] * (picks + 1)), *([stats] * (picks + 1)))


MESH = pl.DeviceIdType.MESH
CHUNKS = 4
RING = 4
VMEM_BYTES = 65_000_000


def crossed(a, b, bits):
    total = 0
    for bit in range(bits):
        total = total + (a // 2**bit + b // 2**bit) % 2 * 2**bit
    return total


def turn_orders(half):
    middle = half // 2
    straight = [middle, middle + 1]

    def hops(turn):
        return (turn // 2).bit_count()

    queues = []
    for first_link in (2, 0):
        turns = [t for t in range(2, half) if t & 2 == first_link and t not in straight]
        outer = sorted(
            (t for t in turns if t >= middle), key=lambda t: (hops(t), t % 2, -t)
        )
        inner = sorted((t for t in turns if t < middle), key=lambda t: (t % 2, hops(t), t))
        queue = [t for both in zip(outer, inner) for t in both]
        queue += outer[len(inner) :] + inner[len(outer) :]
        queues += [((2 * i + 1) / len(queue), turn) for i, turn in enumerate(queue)]
    turned = [turn for _, turn in sorted(queues)]
    late = sorted(
        range(middle, half), key=lambda t: (hops(t) > 2, t % 2, hops(t), -t)
    )
    return straight, turned + [1], [0, 1] + straight + turned, list(range(middle)) + late


def listed(item, values):
    result = values[-1]
    for index, value in enumerate(values[:-1]):
        result = jnp.where(item == index, value, result)
    return result


def attend(take_query, keys, values, store_out, store_stat, group, mask):
    block, width = keys.shape
    factor = width**-0.5 * math.log2(math.e)
    values_t = values.T
    for member in range(group):
        scores = lax.dot_general(
            keys,
            take_query(member),
            (((1,), (1,)), ((), ())),
            preferred_element_type=jnp.float32,
        )
        if mask is not None:
            scores = jnp.where(mask, scores, -jnp.inf)
        top = jnp.max(scores, axis=0, keepdims=True) * factor
        weights = jnp.exp2(scores * factor - top)
        store_stat(member, top, jnp.sum(weights, axis=0, keepdims=True))
        store_out(
            member,
            jnp.dot(
                values_t, weights.astype(jnp.bfloat16), preferred_element_type=jnp.float32
            ).astype(jnp.bfloat16),
        )


def exchange_kernel(
    heads,
    group,
    slots,
    ask_ref,
    queries_hbm,
    span_keys_hbm,
    span_values_hbm,
    past_keys_hbm,
    past_values_hbm,
    outs_hbm,
    stats_ref,
    query,
    near_keys,
    near_values,
    own,
    stage_own,
    stage_far,
    got_own,
    got_far,
    out_buf,
    told,
    told_scalar,
    mine,
    *rest,
):
    mirror, sems = rest[:CHUNKS], rest[CHUNKS:]
    (load_sem, query_sem, out_sem, tell_send, tell_recv, tell_local, copy_send, copy_recv) = sems[:8]
    (own_send, own_recv, far_send, far_recv, whole_send, whole_recv) = sems[8:]
    count = lax.axis_size("seq")
    me = lax.axis_index("seq")
    half = ask_ref.shape[0]
    bits = half.bit_length() - 1
    middle = half // 2
    straight, turned, own_order, far_order = turn_orders(half)
    forward_at = (half // 8, 3 * half // 8, 9 * half // 16, 3 * half // 4)
    local = me % half
    base = me - local
    partner = (me + half) % count
    local_blocks = past_keys_hbm.shape[0]
    block, width = got_own.shape[-2:]
    part = block // CHUNKS
    rows = outs_hbm.shape[0] - count * slots

    def peer(turn):
        return base + crossed(local, turn, bits)

    def load_own(kind, head):
        source = (past_keys_hbm, past_values_hbm)[kind]
        lanes = pl.ds(pl.multiple_of(head * width, width), width)
        return pltpu.make_async_copy(
            source.at[:, 0, :, lanes], own.at[kind, :, head], load_sem.at[kind, head]
        )

    def load_near(kind, head):
        source, target = ((span_keys_hbm, near_keys), (span_values_hbm, near_values))[kind]
        lanes = pl.ds(pl.multiple_of(head * width, width), width)
        return pltpu.make_async_copy(
            source.at[:, :, lanes], target.at[head], load_sem.at[2 + kind, head]
        )

    def load_query(item):
        lanes = pl.ds(pl.multiple_of(item * width, width), width)
        return pltpu.make_async_copy(
            queries_hbm.at[:, :, lanes], query.at[item], query_sem.at[item]
        )

    def each_head(body):
        def step(head, carry):
            for kind in range(2):
                body(kind, head)
            return carry

        lax.fori_loop(0, heads, step, 0)

    def each_query(body):
        def step(item, carry):
            body(item)
            return carry

        lax.fori_loop(0, heads * group, step, 0)

    each_head(lambda kind, head: load_own(kind, head).start())

    barrier = pltpu.get_barrier_semaphore()

    def greet(turn, carry):
        pl.semaphore_signal(barrier, inc=1, device_id=(peer(turn),), device_id_type=MESH)
        return carry

    lax.fori_loop(1, half, greet, 0)
    pl.semaphore_signal(barrier, inc=1, device_id=(partner,), device_id_type=MESH)
    pl.semaphore_wait(barrier, half)

    def tell(turn):
        return pltpu.make_async_remote_copy(
            src_ref=ask_ref.at[turn],
            dst_ref=told.at[turn],
            send_sem=tell_send.at[turn],
            recv_sem=tell_recv.at[turn],
            device_id=(peer(turn),),
            device_id_type=MESH,
        )

    def mirror_copy(chunk, kind):
        return pltpu.make_async_remote_copy(
            src_ref=own.at[kind, :, :, pl.ds(chunk * part, part), :],
            dst_ref=mirror[chunk].at[kind],
            send_sem=copy_send.at[chunk * 2 + kind],
            recv_sem=copy_recv.at[chunk * 2 + kind],
            device_id=(partner,),
            device_id_type=MESH,
        )

    def send_own(turn):
        return pltpu.make_async_remote_copy(
            src_ref=stage_own.at[turn],
            dst_ref=got_own.at[turn],
            send_sem=own_send.at[turn],
            recv_sem=own_recv.at[turn],
            device_id=(peer(turn),),
            device_id_type=MESH,
        )

    def send_whole(turn, slot):
        return pltpu.make_async_remote_copy(
            src_ref=stage_far.at[turn, slot],
            dst_ref=got_far.at[turn, slot],
            send_sem=whole_send.at[turn, slot],
            recv_sem=whole_recv.at[turn, slot],
            device_id=(peer(turn),),
            device_id_type=MESH,
        )

    def send_far(chunk, turn):
        span = pl.ds(chunk * part, part)
        return pltpu.make_async_remote_copy(
            src_ref=stage_far.at[turn, :, :, span, :],
            dst_ref=got_far.at[turn, :, :, span, :],
            send_sem=far_send.at[chunk, turn],
            recv_sem=far_recv.at[chunk, turn],
            device_id=(peer(turn),),
            device_id_type=MESH,
        )

    def each_slot(body):
        def both(turn):
            for slot in range(slots):
                body(turn, slot)

        return both

    def each_turn(first, body, last=half):
        def step(turn, carry):
            body(turn)
            return carry

        lax.fori_loop(first, last, step, 0)

    each_turn(1, lambda turn: tell(turn).start())
    each_head(lambda kind, head: load_own(kind, head).wait())
    def start_mirror(chunk):
        for kind in range(2):
            mirror_copy(chunk, kind).start()

    start_mirror(0)

    each_head(lambda kind, head: load_near(kind, head).start())
    each_query(lambda item: load_query(item).start())
    each_turn(1, lambda turn: tell(turn).wait_recv())
    own_row = pltpu.make_async_copy(ask_ref.at[0], told_scalar.at[0], tell_local.at[0])
    other_rows = pltpu.make_async_copy(
        told.at[pl.ds(1, half - 1)], told_scalar.at[pl.ds(1, half - 1)], tell_local.at[1]
    )
    my_rows = pltpu.make_async_copy(ask_ref, mine, tell_local.at[2])
    for copy in (own_row, other_rows, my_rows):
        copy.start()
    for copy in (own_row, other_rows, my_rows):
        copy.wait()
    def wanted(turn, slot):
        return told_scalar[turn, 0, slot], told_scalar[turn, 0, 2 * slots + slot]

    def gather_own(store, turn):
        for slot in range(slots):
            which, head = wanted(turn, slot)
            for kind in range(2):
                store[turn, slot, kind] = own[kind, which, head]

    def gather_far(chunk, store, turn):
        for slot in range(slots):
            which, head = wanted(turn, slots + slot)
            for kind in range(2):
                store[turn, slot, kind, pl.ds(chunk * part, part), :] = mirror[chunk][
                    kind, which, head
                ]

    gather_own(got_own, 0)
    each_turn(1, functools.partial(gather_own, stage_own))
    for turn in straight:
        send_own(turn).start()
    for chunk in range(1, CHUNKS):
        start_mirror(chunk)
    for turn in turned:
        send_own(turn).start()

    def put_out(place, buffer):
        return pltpu.make_async_copy(out_buf.at[buffer], outs_hbm.at[place], out_sem.at[buffer])

    def pair(place, buffer, first, head, query_block, keys, values, mask):
        if first is not False:
            pl.when(jnp.logical_not(first))(put_out(place, buffer).wait)
        else:
            put_out(place, buffer).wait()

        def take_query(member):
            return query[head * group + member, query_block]

        def store_out(member, value):
            out_buf[buffer, :, pl.ds(member * block, block)] = value

        def store_stat(member, top, total):
            stats_ref[place, 0:1, pl.ds(member * block, block)] = top
            stats_ref[place, 1:2, pl.ds(member * block, block)] = total

        attend(take_query, keys, values, store_out, store_stat, group, mask)
        put_out(place, buffer).start()

    each_head(lambda kind, head: load_near(kind, head).wait())
    each_query(lambda item: load_query(item).wait())
    mask = lax.broadcasted_iota(jnp.int32, (block, block), 0) <= lax.broadcasted_iota(
        jnp.int32, (block, block), 1
    )

    def near_step(item, carry):
        for buffer in range(2):
            row = item * 2 + buffer
            query_block, head = row // heads, row % heads
            pair(
                count * slots + row,
                buffer,
                item == 0,
                head,
                query_block,
                near_keys[head, query_block],
                near_values[head, query_block],
                mask,
            )
        return carry

    lax.fori_loop(0, rows // 2, near_step, 0)

    def far_pair(turn, extra, slot, store):
        place = turn * (2 * slots) + extra + slot
        pair(
            place,
            slot % 2,
            False,
            mine[turn, 0, 2 * slots + extra + slot],
            mine[turn, 0, 4 * slots + extra + slot],
            store[turn, slot, 0],
            store[turn, slot, 1],
            None,
        )

    def forward(chunk):
        for kind in range(2):
            mirror_copy(chunk, kind).wait_recv()
        gather_far(chunk, got_far, 0)
        each_turn(1, functools.partial(gather_far, chunk, stage_far))
        each_turn(1, lambda turn: send_far(chunk, turn).start(), middle)
        if chunk == CHUNKS - 1:
            each_turn(middle, each_slot(lambda turn, slot: send_whole(turn, slot).start()))

    def own_step(item, carry):
        for chunk, place in enumerate(forward_at):
            pl.when(item == place)(functools.partial(forward, chunk))
        turn = listed(item, own_order)

        @pl.when(turn > 0)
        def _():
            send_own(turn).wait_recv()

        for slot in range(slots):
            far_pair(turn, 0, slot, got_own)
        return carry

    lax.fori_loop(0, half, own_step, 0)

    def far_step(item, carry):
        turn = listed(item, far_order)

        @pl.when(jnp.logical_and(turn > 0, turn < middle))
        def _():
            for chunk in range(CHUNKS):
                send_far(chunk, turn).wait_recv()

        for slot in range(slots):
            pl.when(turn >= middle)(send_whole(turn, slot).wait_recv)
            far_pair(turn, slots, slot, got_far)
        return carry

    lax.fori_loop(0, half, far_step, 0)

    for buffer in range(2):
        put_out(buffer, buffer).wait()
    each_turn(1, lambda turn: tell(turn).wait_send())
    each_turn(1, lambda turn: send_own(turn).wait_send())
    for chunk in range(CHUNKS):
        for kind in range(2):
            mirror_copy(chunk, kind).wait_send()
        each_turn(1, lambda turn: send_far(chunk, turn).wait_send(), middle)
    each_turn(middle, each_slot(lambda turn, slot: send_whole(turn, slot).wait_send()))


def join_kernel(
    group, picks, near_place, heads, places_ref, outs_hbm, stats, result_hbm, ring, made, in_sem, out_sem
):
    width, block = outs_hbm.shape[1], outs_hbm.shape[2] // group
    depth = ring.shape[0]
    rows = outs_hbm.shape[0] - near_place

    def places_of(row):
        return [places_ref[row * picks + pick] for pick in range(picks)] + [near_place + row]

    def fetches(row):
        slot = row % depth
        return [
            pltpu.make_async_copy(
                outs_hbm.at[place], ring.at[slot, item], in_sem.at[slot, item]
            )
            for item, place in enumerate(places_of(row))
        ]

    def put(row):
        lanes = pl.ds(pl.multiple_of(row % heads * (group * width), width), group * width)
        lines = pl.ds(pl.multiple_of(row // heads * block, block), block)
        return pltpu.make_async_copy(
            made.at[row % 2], result_hbm.at[lines, lanes], out_sem.at[row % 2]
        )

    def start(row):
        for copy in fetches(row):
            copy.start()

    for row in range(depth - 1):
        start(row)

    def step(row, carry):
        pl.when(row + depth - 1 < rows)(lambda: start(row + depth - 1))
        for copy in fetches(row):
            copy.wait()
        pl.when(row >= 2)(lambda: put(row - 2).wait())
        stat_places = places_of(row)
        for member in range(group):
            span = pl.ds(member * block, block)
            tops = [stats[place, 0:1, span] for place in stat_places]
            top = functools.reduce(jnp.maximum, tops)
            scales = [jnp.exp2(one - top) for one in tops]
            total = sum(
                scale * stats[place, 1:2, span] for scale, place in zip(scales, stat_places)
            )
            inverse = 1.0 / total
            mixed = sum(
                ring[row % depth, item, :, span].astype(jnp.float32) * (scale * inverse)
                for item, scale in enumerate(scales)
            )
            made[row % 2, :, pl.ds(member * width, width)] = mixed.astype(jnp.bfloat16).T
        put(row).start()
        return carry

    lax.fori_loop(0, rows, step, 0)
    for row in (rows - 2, rows - 1):
        put(row).wait()


def mirrored_shards(queries, span_keys, span_values, past_keys, past_values, selected):
    count = lax.axis_size("seq")
    me = lax.axis_index("seq")
    local_blocks, heads, picks = selected.shape
    needed = local_blocks * heads * picks
    rows = local_blocks * heads
    slots = needed // count
    half = count // 2
    block = queries.shape[0] // local_blocks
    width = past_keys.shape[-1] // heads
    group = queries.shape[1] // (heads * width)
    span = group * block
    kind = past_keys.dtype

    chosen = selected.reshape(-1)
    owners = chosen % count
    away = (owners // half != me // half).astype(jnp.int32)
    turns = (owners % half) ^ (me % half)
    places = turns * (2 * slots) + away * slots + owner_ranks(owners)
    found = jnp.arange(needed, dtype=jnp.int32)[:, None] == places[None, :]
    head_flat = lax.broadcasted_iota(jnp.int32, selected.shape, 1).reshape(-1)
    query_blocks = lax.broadcasted_iota(jnp.int32, selected.shape, 0).reshape(-1)

    def placed(values):
        return jnp.sum(jnp.where(found, values[None, :], 0), axis=1).astype(jnp.int32)

    ask = jnp.concatenate(
        [
            placed(item).reshape(half, 1, 2 * slots)
            for item in (chosen // count, head_flat, query_blocks)
        ]
        + [jnp.zeros((half, 1, 128 - 6 * slots), jnp.int32)],
        axis=2,
    )

    total = count * slots + rows
    store = pltpu.VMEM((half, slots, 2, block, width), kind)
    dma = pltpu.SemaphoreType.DMA
    outs, stats = pl.pallas_call(
        functools.partial(exchange_kernel, heads, group, slots),
        in_specs=[pl.BlockSpec(memory_space=pltpu.VMEM)]
        + [pl.BlockSpec(memory_space=pl.ANY)] * 5,
        out_specs=[
            pl.BlockSpec(memory_space=pl.ANY),
            pl.BlockSpec(memory_space=pltpu.VMEM),
        ],
        out_shape=[
            jax.ShapeDtypeStruct((total, width, span), jnp.bfloat16),
            jax.ShapeDtypeStruct((total, 2, span), jnp.float32),
        ],
        scratch_shapes=[
            pltpu.VMEM((heads * group, local_blocks, block, width), queries.dtype),
            pltpu.VMEM((heads, local_blocks, block, width), span_keys.dtype),
            pltpu.VMEM((heads, local_blocks, block, width), span_values.dtype),
            pltpu.VMEM((2, past_keys.shape[0], heads, block, width), kind),
            store,
            store,
            store,
            store,
            pltpu.VMEM((2, width, span), jnp.bfloat16),
            pltpu.VMEM((half, 1, 128), jnp.int32),
            pltpu.SMEM((half, 1, 128), jnp.int32),
            pltpu.SMEM((half, 1, 128), jnp.int32),
        ]
        + [pltpu.VMEM((2, past_keys.shape[0], heads, block // CHUNKS, width), kind)] * CHUNKS
        + [
            dma((4, heads)),
            dma((heads * group,)),
            dma((2,)),
            dma((half,)),
            dma((half,)),
            dma((3,)),
            dma((2 * CHUNKS,)),
            dma((2 * CHUNKS,)),
            dma((half,)),
            dma((half,)),
            dma((CHUNKS, half // 2)),
            dma((CHUNKS, half // 2)),
            dma((half, slots)),
            dma((half, slots)),
        ],
        compiler_params=pltpu.CompilerParams(
            collective_id=0, has_side_effects=True, vmem_limit_bytes=VMEM_BYTES
        ),
    )(
        ask,
        queries.reshape(local_blocks, block, -1),
        span_keys.reshape(local_blocks, block, -1),
        span_values.reshape(local_blocks, block, -1),
        past_keys,
        past_values,
    )

    return pl.pallas_call(
        functools.partial(join_kernel, group, picks, count * slots, heads),
        in_specs=[
            pl.BlockSpec(memory_space=pltpu.SMEM),
            pl.BlockSpec(memory_space=pl.ANY),
            pl.BlockSpec(memory_space=pltpu.VMEM),
        ],
        out_specs=pl.BlockSpec(memory_space=pl.ANY),
        out_shape=jax.ShapeDtypeStruct(queries.shape, queries.dtype),
        scratch_shapes=[
            pltpu.VMEM((RING, picks + 1, width, span), jnp.bfloat16),
            pltpu.VMEM((2, block, group * width), jnp.bfloat16),
            dma((RING, picks + 1)),
            dma((2,)),
        ],
        compiler_params=pltpu.CompilerParams(vmem_limit_bytes=VMEM_BYTES),
    )(places, outs, stats)


def shards(queries, span_keys, span_values, past_keys, past_values, selected):
    count = lax.axis_size("seq")
    needed = selected.size
    half = count // 2
    held = 2 * (queries.size + 2 * span_keys.size + 4 * past_keys.size)
    held += 16 * needed * past_keys.shape[2] * (past_keys.shape[3] // selected.shape[1]) // 2
    fits = held < VMEM_BYTES - 2**23
    whole = needed == count * max(needed // count, 1) and needed // max(count, 1) == 2
    if fits and whole and half >= 2 * CHUNKS and half & (half - 1) == 0:
        call = mirrored_shards
    else:
        call = plain_shards
    return call(queries, span_keys, span_values, past_keys, past_values, selected)


def solution(mesh):
    return jax.shard_map(
        shards,
        mesh=mesh,
        in_specs=(
            P("seq", None),
            P("seq", None),
            P("seq", None),
            P(None, "seq", None, None),
            P(None, "seq", None, None),
            P("seq", None, None),
        ),
        out_specs=P("seq", None),
        check_vma=False,
    )
```
